32 devices in a mesh: gx: 4 (over x, core), gy: 4 (over z), gz: 2 (over y).
Axes of the slice: x: 2, y: 2, z: 4, core: 2. Of those that a mesh axis runs over, the one named last changes fastest.
Arguments:
- density: float32 [16, 128, 256], P('gx', 'gy', 'gz'), may hold values from 0.5 to 2
- velocity: float32 [3, 16, 128, 256], P(None, 'gx', 'gy', 'gz'), may hold values from -2.5 to 2.5
- pressure: float32 [16, 128, 256], P('gx', 'gy', 'gz'), may hold values from 0.5 to 2
Outputs:
- section_state: float32 [5, 16, 128, 256], P(None, 'gx', 'gy', 'gz')
The draws below stay inside these ranges and needn't reach their ends.
All inputs are finite; a program needn't handle non-finite values.
Results may differ from the reference program's by a relative error of at most 0.0003.
Values sent between devices are 32-bit elements; how exact they have to be, the bound alone decides.
A program may use at most 64 MiB of HBM per device.

```python
import math
import jax
import jax.numpy as jnp
from jax import lax

CX = 4
NX = 16
NY = 128
NZ = 256


def draw_velocity(key, part):
    growth = 1.0 + 2.0 * jnp.arange(NX, dtype=jnp.float32) / NX
    growth = growth[None, :, None, None]
    sample = jnp.clip(jax.random.normal(key, (3, NX, NY, NZ), jnp.float32), -2.5, 2.5)
    return 0.3 * growth * sample


def shard_levels(stream_key, shape, split, least, high):
    loudness = 1.0
    for position, shards_of in split:
        steps = jax.random.uniform(jax.random.fold_in(jax.random.fold_in(stream_key, 6), position), (shards_of,), jnp.float32, least / len(split), high / len(split))
        loudness = loudness * jnp.repeat(jnp.exp(steps), shape[position] // shards_of).reshape((-1,) + (1,) * (len(shape) - 1 - position))
    return loudness


def setup_inputs(seed: int = 0) -> dict:
    keys = jax.random.split(jax.random.key(seed), 4)
    return {
        "density": jnp.clip(jnp.exp(math.log(2.0) - 1.3862944 * jax.random.uniform(keys[0], (NX, NY, NZ), jnp.float32) ** shard_levels(keys[0], (NX, NY, NZ), ((0, 4), (1, 4), (2, 2)), -0.2, 0.2)), 0.5, 2.0),
        "velocity": draw_velocity(jax.random.fold_in(keys[3], 71), 0),
        "pressure": jnp.clip(jnp.exp(math.log(2.0) - 1.3862944 * jax.random.uniform(keys[2], (NX, NY, NZ), jnp.float32) ** shard_levels(keys[2], (NX, NY, NZ), ((0, 4), (1, 4), (2, 2)), -0.2, 0.2)), 0.5, 2.0),
    }


gamma_gas = 1.4
weno_eps = 1e-06
cfl_number = 0.4

def conserved(density, velocity, pressure):
    momenta = density[None] * velocity
    kinetic = 0.5 * density * lax.optimization_barrier(jnp.sum(velocity * velocity, axis=0))
    energy = pressure / (gamma_gas - 1.0) + kinetic
    return jnp.concatenate([density[None], momenta, energy[None]], axis=0)

def wave_speed(density, velocity, pressure):
    sound = jnp.sqrt(gamma_gas * pressure / density)
    return jnp.max(lax.optimization_barrier(jnp.sum(jnp.abs(velocity), axis=0)) + 3.0 * sound)

def combine(coeffs, arrays):
    total = None
    for coeff, array in zip(coeffs, arrays):
        if isinstance(coeff, float) and coeff == 0.0:
            continue
        term = coeff * array
        total = term if total is None else total + term
    return total

def weno_face(values):
    first, second, third, fourth, fifth = values
    cand_left = (2.0 * first - 7.0 * second + 11.0 * third) / 6.0
    cand_middle = (-second + 5.0 * third + 2.0 * fourth) / 6.0
    cand_right = (2.0 * third + 5.0 * fourth - fifth) / 6.0
    smooth_left = 13.0 / 12.0 * (first - 2.0 * second + third) ** 2 + 0.25 * (first - 4.0 * second + 3.0 * third) ** 2
    smooth_middle = 13.0 / 12.0 * (second - 2.0 * third + fourth) ** 2 + 0.25 * (second - fourth) ** 2
    smooth_right = 13.0 / 12.0 * (third - 2.0 * fourth + fifth) ** 2 + 0.25 * (3.0 * third - 4.0 * fourth + fifth) ** 2
    weight_left = 0.1 / (weno_eps + smooth_left) ** 2
    weight_middle = 0.6 / (weno_eps + smooth_middle) ** 2
    weight_right = 0.3 / (weno_eps + smooth_right) ** 2
    return (weight_left * cand_left + weight_middle * cand_middle + weight_right * cand_right) / (weight_left + weight_middle + weight_right)

def direction_flux(padded, field_dim, normal_comp):
    cells = padded.shape[field_dim + 1] - 6
    faces = cells + 1
    density = padded[0]
    energy = padded[4]
    velocity = [padded[1 + member] / density for member in range(3)]
    speed_sq = velocity[0] * velocity[0] + velocity[1] * velocity[1] + velocity[2] * velocity[2]
    pressure = (gamma_gas - 1.0) * (energy - 0.5 * density * speed_sq)
    sound_sq = gamma_gas * pressure / density
    sound = jnp.sqrt(sound_sq)
    enthalpy = (energy + pressure) / density
    normal_vel = velocity[normal_comp]
    others = [member for member in range(3) if member != normal_comp]
    order = [0, 1 + normal_comp, 1 + others[0], 1 + others[1], 4]
    state_perm = [padded[member] for member in order]
    flux_perm = [density * normal_vel, padded[1 + normal_comp] * normal_vel + pressure, padded[1 + others[0]] * normal_vel, padded[1 + others[1]] * normal_vel, (energy + pressure) * normal_vel]
    signal = jnp.abs(normal_vel) + sound

    def window(array, offset):
        return lax.slice_in_dim(array, offset, offset + faces, axis=field_dim)
    root_left = jnp.sqrt(window(density, 2))
    root_right = jnp.sqrt(window(density, 3))
    share_left = root_left / (root_left + root_right)
    share_right = root_right / (root_left + root_right)
    roe_vel = [share_left * window(member, 2) + share_right * window(member, 3) for member in velocity]
    roe_enth = share_left * window(enthalpy, 2) + share_right * window(enthalpy, 3)
    jump_sq = sum(((window(member, 3) - window(member, 2)) ** 2 for member in velocity))
    roe_sound_sq = share_left * window(sound_sq, 2) + share_right * window(sound_sq, 3) + 0.5 * (gamma_gas - 1.0) * share_left * share_right * jump_sq
    roe_sound = jnp.sqrt(roe_sound_sq)
    normal_roe = roe_vel[normal_comp]
    tang_first = roe_vel[others[0]]
    tang_second = roe_vel[others[1]]
    roe_qsq = normal_roe * normal_roe + tang_first * tang_first + tang_second * tang_second
    b_one = (gamma_gas - 1.0) / roe_sound_sq
    b_two = 0.5 * b_one * roe_qsq
    inv_sound = 1.0 / roe_sound
    left_rows = [[0.5 * (b_two + normal_roe * inv_sound), -0.5 * (b_one * normal_roe + inv_sound), -0.5 * b_one * tang_first, -0.5 * b_one * tang_second, 0.5 * b_one], [1.0 - b_two, b_one * normal_roe, b_one * tang_first, b_one * tang_second, -b_one], [-tang_first, 0.0, 1.0, 0.0, 0.0], [-tang_second, 0.0, 0.0, 1.0, 0.0], [0.5 * (b_two - normal_roe * inv_sound), -0.5 * (b_one * normal_roe - inv_sound), -0.5 * b_one * tang_first, -0.5 * b_one * tang_second, 0.5 * b_one]]
    right_rows = [[1.0, 1.0, 0.0, 0.0, 1.0], [normal_roe - roe_sound, normal_roe, 0.0, 0.0, normal_roe + roe_sound], [tang_first, tang_first, 1.0, 0.0, tang_first], [tang_second, tang_second, 0.0, 1.0, tang_second], [roe_enth - normal_roe * roe_sound, 0.5 * roe_qsq, tang_first, tang_second, roe_enth + normal_roe * roe_sound]]
    alpha = window(signal, 0)
    for offset in range(1, 6):
        alpha = jnp.maximum(alpha, window(signal, offset))
    plus_vals = [[None] * 6 for member in range(5)]
    minus_vals = [[None] * 6 for member in range(5)]
    for offset in range(6):
        state_here = [window(member, offset) for member in state_perm]
        flux_here = [window(member, offset) for member in flux_perm]
        for charac in range(5):
            char_state = combine(left_rows[charac], state_here)
            char_flux = combine(left_rows[charac], flux_here)
            plus_vals[charac][offset] = 0.5 * (char_flux + alpha * char_state)
            minus_vals[charac][offset] = 0.5 * (char_flux - alpha * char_state)
    hats = []
    for charac in range(5):
        upwind = weno_face(plus_vals[charac][0:5])
        downwind = weno_face([minus_vals[charac][5], minus_vals[charac][4], minus_vals[charac][3], minus_vals[charac][2], minus_vals[charac][1]])
        hats.append(upwind + downwind)
    face_flux = [None] * 5
    for member in range(5):
        face_flux[order[member]] = combine(right_rows[member], hats)
    result = [lax.slice_in_dim(member, 1, faces, axis=field_dim) - lax.slice_in_dim(member, 0, faces - 1, axis=field_dim) for member in face_flux]
    return jnp.stack(result, axis=0)

def reference(density, velocity, pressure):
    state = conserved(density, velocity, pressure)
    step = cfl_number / wave_speed(density, velocity, pressure)
    padded = jnp.pad(state, ((0, 0), (3, 3), (3, 3), (3, 3)), mode='wrap')

    def slab_update(start):
        piece = lax.dynamic_slice_in_dim(padded, start, CX + 6, axis=1)
        total = direction_flux(piece[:, :, 3:-3, 3:-3], 0, 0)
        total = total + direction_flux(piece[:, 3:-3, :, 3:-3], 1, 1)
        total = total + direction_flux(piece[:, 3:-3, 3:-3, :], 2, 2)
        return total
    starts = jnp.arange(NX // CX, dtype=jnp.int32) * CX
    slabs = lax.map(slab_update, starts)
    total = jnp.moveaxis(slabs, 0, 1).reshape(5, NX, NY, NZ)
    return state - step * total
```

```python
import functools
import math

import jax
import jax.numpy as jnp
from jax import lax
from jax.experimental import pallas as pl
from jax.experimental.pallas import tpu as pltpu
from jax.sharding import PartitionSpec as P

MESH = pl.DeviceIdType.MESH
AXES = ("gx", "gy", "gz")
gamma_gas = 1.4
weno_eps = 1e-06
cfl_number = 0.4
scale = 0.125
eps_outer = 0.75 * 16.0 * scale * scale * weno_eps
eps_inner = 0.75 * 4.0 * scale * scale * weno_eps
ROWS = 8
AHEAD = 8


def rcp(x):
    guess = pl.reciprocal(x, approx=True)
    return guess * (2.0 - x * guess)


def cell_basis(rho, v, p):
    inv_root = lax.rsqrt(rho)
    c2 = gamma_gas * p * (inv_root * inv_root)
    m = [rho * u for u in v]
    energy = 2.5 * p + 0.5 * (m[0] * v[0] + m[1] * v[1] + m[2] * v[2])
    return rho, v, p, m, energy, rho * inv_root, c2, c2 * lax.rsqrt(c2)


def cell_arrays(basis, order):
    rho, v, p, m, energy, root, c2, sound = basis
    vn, va, vb = [v[k] for k in order]
    mn, ma, mb = [m[k] for k in order]
    return [
        rho, mn, ma, mb, energy,
        mn * vn + p, ma * vn, mb * vn, (energy + p) * vn,
        root, vn, va, vb, c2, jnp.abs(vn) + sound,
    ]


FIRST, SECOND, THIRD = (0, 1, 2), (1, 0, 2), (2, 0, 1)


def put_cells(ref, row, arrays):
    for k, array in enumerate(arrays):
        ref[k, pl.ds(row, array.shape[0]), :] = array


def weno(d1, d2, d3, d4, eps):
    h2 = (d2 + d2) - d1
    h3 = (d3 + d3) - d4
    e1, e2, e3 = d2 - d1, d3 - d2, d4 - d3
    s2, s3 = 0.75 * d2, 0.75 * d3
    a = (e1 * e1 + s2 * h2) + eps
    b = (e2 * e2 + s2 * d3) + eps
    c = (e3 * e3 + s3 * h3) + eps
    bc, ac, ab = b * c, a * c, a * b
    w0 = bc * bc
    w1 = 6.0 * (ac * ac)
    w2 = 1.5 * (ab * ab)
    den = w0 + w1 + (w2 + w2)
    return (w0 * (h2 - d3) + w2 * (h3 - d2)) * rcp(den)


def face_tile(cells, flux, base, stride, row, rows=ROWS, step=None):
    def load(k, j):
        return cells[k, pl.ds(base + j * stride, rows, step), :]

    sl, sr = load(9, 2), load(9, 3)
    inv = rcp(sl + sr)
    wl, wr = sl * inv, sr * inv
    vl = [load(10 + k, 2) for k in range(3)]
    dv = [load(10 + k, 3) - vl[k] for k in range(3)]
    un, ta, tb = [vl[k] + wr * dv[k] for k in range(3)]
    jump = dv[0] * dv[0] + dv[1] * dv[1] + dv[2] * dv[2]
    c2 = wl * load(13, 2) + wr * load(13, 3) + (0.2 * (wl * wr)) * jump
    ic = lax.rsqrt(c2)
    sound = c2 * ic
    b1 = 0.4 * (ic * ic)
    qh = 0.5 * (un * un + ta * ta + tb * tb)
    enth = 2.5 * c2 + qh
    alpha = load(14, 0)
    for j in range(1, 6):
        alpha = jnp.maximum(alpha, load(14, j))

    state = [[load(k, j) for j in range(6)] for k in range(5)]
    phys = [state[1]] + [[load(k, j) for j in range(6)] for k in range(5, 9)]
    du = [[s[j + 1] - s[j] for j in range(5)] for s in state]
    df = [du[1]] + [[s[j + 1] - s[j] for j in range(5)] for s in phys[1:]]
    au = [[alpha * d for d in s] for s in du]

    def project(r, mn, ma, mb, e):
        s = (un * r - mn) * ic
        z = b1 * (e - un * mn - ta * ma - tb * mb + qh * r)
        return z + s, r - z, ma - ta * r, mb - tb * r, z - s

    plus = [project(*[df[k][j] + au[k][j] for k in range(5)]) for j in range(4)]
    minus = [project(*[df[k][j] - au[k][j] for k in range(5)]) for j in range(1, 5)]
    hats = []
    for k in range(5):
        eps = eps_outer if k in (0, 4) else eps_inner
        up = weno(plus[0][k], plus[1][k], plus[2][k], plus[3][k], eps)
        down = weno(minus[3][k], minus[2][k], minus[1][k], minus[0][k], eps)
        hats.append(up - down)
    lin = []
    for k in range(5):
        centre = 6.0 * (phys[k][2] + phys[k][3]) + (df[k][1] - df[k][3])
        lin.append(centre + ((au[k][1] + au[k][3]) - (au[k][2] + au[k][2])))
    h1, h2, h3, h4, h5 = hats
    h2, h3, h4 = h2 + h2, h3 + h3, h4 + h4
    h15 = h1 + h5
    k5 = sound * (h5 - h1)
    s = h15 + h2
    result = [
        lin[0] + s,
        lin[1] + (un * s + k5),
        lin[2] + (ta * s + h3),
        lin[3] + (tb * s + h4),
        lin[4] + (enth * h15 + un * k5 + qh * h2 + ta * h3 + tb * h4),
    ]
    for k in range(5):
        flux[k, pl.ds(row, rows, step), :] = result[k]


def is_star(counts):
    return math.prod(counts) <= 64 and counts[0] >= 2 and counts[1] >= 3 and counts[2] >= 2


def kernel(
    counts, den_in, vel_in, pre_in, out,
    raw, cx, cy, cz, gx, gy, gz, acc, tz, hx, sy, hy, hz, top, got,
    in_sem, x_send, x_recv, y_send, y_recv, z_send, z_recv, top_send, top_recv, cast_send, cast_recv,
):
    nx, ny, lanes = raw.shape[1:]
    nrow = nx * ny
    nz = lanes
    tiles = ny // ROWS
    ypad = ny + 2 * ROWS
    devices = math.prod(counts)
    star = is_star(counts)

    pairs = ((den_in, raw.at[0]), (vel_in, raw.at[pl.ds(1, 3)]), (pre_in, raw.at[4]))
    loads = [pltpu.make_async_copy(a, b, in_sem.at[k]) for k, (a, b) in enumerate(pairs)]
    for copy in loads:
        copy.start()

    me = [lax.axis_index(a) for a in AXES]
    rank = (me[0] * counts[1] + me[1]) * counts[2] + me[2]
    roots = (0, counts[1] * counts[2])
    root = jnp.logical_and(me[0] <= 1, jnp.logical_and(me[1] == 0, me[2] == 0))
    odd = lax.rem(me[0], 2)
    last = me[1] == counts[1] - 1

    def device(d):
        return {
            "gx": lax.div(d, counts[1] * counts[2]),
            "gy": lax.rem(lax.div(d, counts[2]), counts[1]),
            "gz": lax.rem(d, counts[2]),
        }

    def near(axis, way):
        return {AXES[axis]: lax.rem(me[axis] + way + counts[axis], counts[axis])}

    barrier = pltpu.get_barrier_semaphore()

    def greet(peer):
        pl.semaphore_signal(barrier, inc=1, device_id=peer, device_id_type=MESH)

    if star:
        greeted = 2
        for axis in (0, 2):
            for way in sorted({1, counts[axis] - 1}):
                greet(near(axis, way))
                greeted += 1
        pl.when(me[1] > 0)(lambda: greet({"gy": me[1] - 1}))
        pl.when(me[1] < counts[1] - 1)(lambda: greet({"gy": me[1] + 1}))
        pl.when(me[1] == 0)(lambda: greet({"gy": counts[1] - 1}))
        greeted = greeted + jnp.where(me[1] == 0, 1, 2) - jnp.where(root, 1, 0)

        @pl.when(root)
        def _():
            @pl.loop(0, devices)
            def _(d):
                pl.when(d != rank)(lambda: greet(device(d)))
    else:
        peers = [(a, {AXES[a]: lax.rem(me[a] + k, counts[a])}) for a in range(3) for k in range(1, counts[a])]
        greeted = len(peers)
        for _, peer in peers:
            greet(peer)

    for copy in loads:
        copy.wait()

    def speeds(i, best):
        for t in range(tiles):
            r = t * ROWS
            inv_root = lax.rsqrt(raw[0, i, pl.ds(r, ROWS), :])
            c2 = gamma_gas * raw[4, i, pl.ds(r, ROWS), :] * (inv_root * inv_root)
            v1, v2, v3 = [jnp.abs(raw[1 + k, i, pl.ds(r, ROWS), :]) for k in range(3)]
            best = jnp.maximum(best, ((v1 + v2) + v3) + 3.0 * (c2 * lax.rsqrt(c2)))
        return best

    best = lax.fori_loop(0, nx, speeds, jnp.zeros((ROWS, lanes), jnp.float32))
    own = jnp.max(best, axis=0, keepdims=True)
    top[0] = own
    if star:
        got[rank] = own

    def own_cells():
        @pl.loop(0, nx)
        def _(i):
            for t in range(tiles):
                r = t * ROWS
                rho, v1, v2, v3, p = [raw[k, i, pl.ds(r, ROWS), :] for k in range(5)]
                basis = cell_basis(scale * rho, (v1, v2, v3), scale * p)
                put_cells(cx, pl.multiple_of((3 + i) * ny + r, ROWS), cell_arrays(basis, FIRST))
                put_cells(cy, pl.multiple_of(i * ypad + ROWS + r, ROWS), cell_arrays(basis, SECOND))

    def stage():
        for side, start in ((0, ny - 3), (1, 0)):
            for i in range(nx):
                for k in range(5):
                    sy[side, pl.ds(3 * (k * nx + i), 3), :] = raw[k, i, pl.ds(start, 3), :]
        for k in range(5):
            tz[k] = raw[k].reshape(nrow, nz).T

    def own_turned():
        @pl.loop(0, nz // ROWS, unroll=4)
        def _(t):
            r = pl.multiple_of(t * ROWS, ROWS)
            rho, v1, v2, v3, p = [tz[k, pl.ds(r, ROWS), :] for k in range(5)]
            basis = cell_basis(scale * rho, (v1, v2, v3), scale * p)
            put_cells(cz, r + ROWS, cell_arrays(basis, THIRD))

    def z_face(t):
        r = pl.multiple_of(t * ROWS, ROWS)
        face_tile(cz, gz, r + 5, 1, r)

    def y_face(i, t):
        face_tile(cy, gy, i * ypad + t * ROWS + 5, 1, pl.multiple_of(i * ypad + t * ROWS, ROWS))

    first = 1
    if star:
        ahead = min(AHEAD, nz // ROWS - 2)

        @pl.when(root)
        def _():
            stage()
            own_turned()
            pl.loop(1, 1 + ahead)(z_face)

        first = 1 + jnp.where(root, ahead, 0)

    pl.semaphore_wait(barrier, greeted)

    def remote(src, dst, send, recv, peer):
        return pltpu.make_async_remote_copy(
            src_ref=src, dst_ref=dst, send_sem=send, recv_sem=recv, device_id=peer, device_id_type=MESH
        )

    def to_root(k):
        return remote(top.at[0], got.at[rank], top_send.at[k], top_recv.at[rank], device(jnp.int32(roots[k])))

    def from_device(d):
        return remote(top.at[0], got.at[d], top_send.at[0], top_recv.at[d], device(d))

    def cast(d):
        return remote(top.at[1], top.at[2], cast_send.at[d], cast_recv.at[0], device(d))

    def exchange(axis):
        return [
            remote(top.at[axis], got.at[slot], top_send.at[slot], top_recv.at[slot], peer)
            for slot, (other, peer) in enumerate(peers) if other == axis
        ]

    def next_top(axis):
        best = top[axis]
        for copy in exchange(axis):
            copy.wait()
        for slot, (other, _) in enumerate(peers):
            if other == axis:
                best = jnp.maximum(best, got[slot])
        top[axis + 1] = best
        if axis < 2:
            for copy in exchange(axis + 1):
                copy.start()

    def x_copy(side, p):
        src = jnp.where(side == 0, nx - 1 - p, p)
        dst = jnp.where(side == 0, 2 - p, p)
        slot = 3 * side + p
        peer = near(0, jnp.where(side == 0, 1, -1))
        return remote(raw.at[:, src], hx.at[side, :, dst], x_send.at[slot], x_recv.at[slot], peer)

    def y_copy(side):
        return remote(sy.at[side], hy.at[side], y_send.at[side], y_recv.at[side], near(1, 1 - 2 * side))

    def z_copy(side):
        start = 0 if side else nz - ROWS
        src = tz.at[:, pl.ds(start, ROWS), :]
        return remote(src, hz.at[side], z_send.at[side], z_recv.at[side], near(2, 1 - 2 * side))

    if star:
        for k in range(2):
            pl.when(rank != roots[k])(lambda: to_root(k).start())
    else:
        for copy in exchange(0):
            copy.start()
    for p in range(3):
        x_copy(1 - odd, p).start()
    for p in range(3):
        x_copy(odd, p).start()
    if star:
        @pl.when(jnp.logical_not(root))
        def _():
            stage()
    else:
        stage()
    z_copy(0).start()
    z_copy(1).start()
    y_copy(0).start()
    if star:
        pl.when(me[1] > 0)(lambda: y_copy(1).start())
        pl.when(jnp.logical_not(root))(own_turned)
    else:
        y_copy(1).start()
        own_turned()
    own_cells()

    lax.fori_loop(first, nz // ROWS - 1, lambda t, c: (z_face(t), c)[1], 0)
    if not star:
        next_top(0)

    @pl.loop(0, nx * (tiles - 2))
    def _(q):
        y_face(q // (tiles - 2), lax.rem(q, tiles - 2) + 1)

    if not star:
        next_top(1)

    def x_plane(side, p):
        x_copy(side, p).wait_recv()
        j = jnp.where(side == 0, 2 - p, p)
        base = jnp.where(side == 0, 2 - p, nx + 3 + p) * ny
        for t in range(tiles):
            r = t * ROWS
            rho, v1, v2, v3, pr = [hx[side, k, j, pl.ds(r, ROWS), :] for k in range(5)]
            basis = cell_basis(scale * rho, (v1, v2, v3), scale * pr)
            put_cells(cx, pl.multiple_of(base + r, ROWS), cell_arrays(basis, FIRST))

    def x_faces(start, number):
        @pl.loop(0, number * tiles)
        def _(q):
            r = pl.multiple_of(start * ny + q * ROWS, ROWS)
            face_tile(cx, gx, r, ny, r)

    pl.loop(0, 3)(lambda p: x_plane(1 - odd, p))
    x_faces(jnp.where(odd == 1, 0, 3), nx - 2)

    for side, row in ((0, 0), (1, nz + ROWS)):
        z_copy(side).wait_recv()
        rho, v1, v2, v3, p = [hz[side, k] for k in range(5)]
        put_cells(cz, row, cell_arrays(cell_basis(scale * rho, (v1, v2, v3), scale * p), THIRD))

    @pl.loop(0, 3)
    def _(t):
        z_face(jnp.where(t == 0, 0, nz // ROWS - 2 + t))

    for k, field in enumerate((0, 3, 1, 2, 4)):
        acc[field] = (gz[k, pl.ds(1, nz), :] - gz[k, pl.ds(0, nz), :]).T

    def y_side(side):
        y_copy(side).wait_recv()
        if side == 0 and star:
            pl.when(me[1] == 0)(lambda: y_copy(1).start())
        for i in range(nx):
            rho, v1, v2, v3, p = [hy[side, pl.ds(3 * (k * nx + i), 3), :] for k in range(5)]
            row = i * ypad + ROWS + (ny if side else -3)
            put_cells(cy, row, cell_arrays(cell_basis(scale * rho, (v1, v2, v3), scale * p), SECOND))

        @pl.loop(0, nx)
        def _(i):
            y_face(i, (tiles - 1) * side)

    def x_next(p):
        x_plane(odd, p)
        x_faces(jnp.where(odd == 1, nx - 2 + p, 2 - p), 1)

    pl.when(last)(lambda: y_side(0))
    pl.when(jnp.logical_not(last))(lambda: y_side(1))
    pl.loop(0, 2)(x_next)
    pl.when(last)(lambda: y_side(1))
    pl.when(jnp.logical_not(last))(lambda: y_side(0))
    face_tile(cy, gy, ny + 5, 1, ny, nx, ypad)

    @pl.loop(0, nx)
    def _(i):
        for t in range(tiles):
            r = t * ROWS
            row = pl.multiple_of(i * ny + r, ROWS)
            yrow = pl.multiple_of(i * ypad + r, ROWS)
            for field, k in enumerate((0, 2, 1, 3, 4)):
                turn = gy[k, pl.ds(yrow + 1, ROWS), :] - gy[k, pl.ds(yrow, ROWS), :]
                acc[field, pl.ds(row, ROWS), :] = acc[field, pl.ds(row, ROWS), :] + turn

    def gather(k):
        @pl.when(rank == roots[k])
        def _():
            @pl.loop(0, devices)
            def _(d):
                pl.when(d != rank)(lambda: from_device(d).wait_recv())

            best = jnp.max(got[...], axis=0)
            top[1] = best
            top[2] = best
            if k == 1:
                @pl.loop(1, devices)
                def _(d):
                    pl.when(d != rank)(lambda: cast(d).start())

    if star:
        gather(1)
    else:
        next_top(2)
    x_next(2)
    if star:
        gather(0)

    @pl.loop(0, nx)
    def _(i):
        for t in range(tiles):
            row = pl.multiple_of(i * ny + t * ROWS, ROWS)
            for field in range(5):
                turn = gx[field, pl.ds(row + ny, ROWS), :] - gx[field, pl.ds(row, ROWS), :]
                acc[field, pl.ds(row, ROWS), :] = acc[field, pl.ds(row, ROWS), :] + turn

    if star:
        pl.when(jnp.logical_not(root))(lambda: cast(rank).wait_recv())
    largest = jnp.max(top[2 if star else 3], axis=(0, 1), keepdims=True)
    factor = jnp.broadcast_to((cfl_number / (12.0 * scale)) / largest, (ROWS, lanes))

    @pl.loop(0, nx)
    def _(i):
        for t in range(tiles):
            r = t * ROWS
            row = pl.multiple_of(i * ny + r, ROWS)
            for field in range(5):
                state = cx[field, pl.ds(pl.multiple_of(row + 3 * ny, ROWS), ROWS), :]
                out[field, i, pl.ds(r, ROWS), :] = (1.0 / scale) * state - factor * acc[field, pl.ds(row, ROWS), :]

    if star:
        for k in range(2):
            pl.when(rank != roots[k])(lambda: to_root(k).wait_send())

        @pl.when(rank == roots[1])
        def _():
            @pl.loop(1, devices)
            def _(d):
                pl.when(d != rank)(lambda: cast(d).wait_send())
    for side in range(2):
        for p in range(3):
            x_copy(side, p).wait_send()
        y_copy(side).wait_send()
        z_copy(side).wait_send()


def local(counts, density, velocity, pressure):
    nx, ny, nz = density.shape
    nrow = nx * ny
    slots = math.prod(counts) if is_star(counts) else sum(counts) - 3
    casts = slots if is_star(counts) else 1
    f32 = jnp.float32
    vmem = pl.BlockSpec(memory_space=pltpu.VMEM)
    edge = pl.cdiv(15 * nx, ROWS) * ROWS
    return pl.pallas_call(
        functools.partial(kernel, counts),
        out_shape=pltpu.VMEM((5, nx, ny, nz), f32),
        in_specs=[pl.BlockSpec(memory_space=pl.ANY)] * 3,
        out_specs=vmem,
        scratch_shapes=[
            pltpu.VMEM((5, nx, ny, nz), f32),
            pltpu.VMEM((15, (nx + 6) * ny + ROWS, nz), f32),
            pltpu.VMEM((15, nx * (ny + 2 * ROWS) + ROWS, nz), f32),
            pltpu.VMEM((15, nz + 3 * ROWS, nrow), f32),
            pltpu.VMEM((5, (nx + 1) * ny, nz), f32),
            pltpu.VMEM((5, nx * (ny + 2 * ROWS), nz), f32),
            pltpu.VMEM((5, nz + ROWS, nrow), f32),
            pltpu.VMEM((5, nrow, nz), f32),
            pltpu.VMEM((5, nz, nrow), f32),
            pltpu.VMEM((2, 5, 3, ny, nz), f32),
            pltpu.VMEM((2, edge, nz), f32),
            pltpu.VMEM((2, edge, nz), f32),
            pltpu.VMEM((2, 5, ROWS, nrow), f32),
            pltpu.VMEM((4, 1, nz), f32),
            pltpu.VMEM((slots, 1, nz), f32),
            pltpu.SemaphoreType.DMA((3,)),
            pltpu.SemaphoreType.DMA((6,)),
            pltpu.SemaphoreType.DMA((6,)),
            pltpu.SemaphoreType.DMA((2,)),
            pltpu.SemaphoreType.DMA((2,)),
            pltpu.SemaphoreType.DMA((2,)),
            pltpu.SemaphoreType.DMA((2,)),
            pltpu.SemaphoreType.DMA((slots,)),
            pltpu.SemaphoreType.DMA((slots,)),
            pltpu.SemaphoreType.DMA((casts,)),
            pltpu.SemaphoreType.DMA((1,)),
        ],
        compiler_params=pltpu.CompilerParams(collective_id=0, has_side_effects=True),
    )(density, velocity, pressure)


def solution(mesh):
    counts = tuple(mesh.shape[a] for a in AXES)
    in_specs = (P("gx", "gy", "gz"), P(None, "gx", "gy", "gz"), P("gx", "gy", "gz"))
    out_specs = P(None, "gx", "gy", "gz")
    return jax.shard_map(
        functools.partial(local, counts), mesh=mesh, in_specs=in_specs, out_specs=out_specs, check_vma=False
    )
```

```python
import functools
import math

import jax
import jax.numpy as jnp
from jax import lax
from jax.experimental import pallas as pl
from jax.experimental.pallas import tpu as pltpu
from jax.sharding import PartitionSpec as P

MESH = pl.DeviceIdType.MESH
AXES = ("gx", "gy", "gz")
gamma_gas = 1.4
weno_eps = 1e-06
cfl_number = 0.4
scale = 0.125
eps_outer = 0.75 * 16.0 * scale * scale * weno_eps
eps_inner = 0.75 * 4.0 * scale * scale * weno_eps
ROWS = 8
AHEAD = 8


def rcp(x):
    return pl.reciprocal(x)


def cell_basis(rho, v, p):
    inv_root = lax.rsqrt(rho)
    c2 = gamma_gas * p * (inv_root * inv_root)
    m = [rho * u for u in v]
    energy = 2.5 * p + 0.5 * (m[0] * v[0] + m[1] * v[1] + m[2] * v[2])
    return rho, v, p, m, energy, rho * inv_root, c2, c2 * lax.rsqrt(c2)


def cell_arrays(basis, order):
    rho, v, p, m, energy, root, c2, sound = basis
    vn, va, vb = [v[k] for k in order]
    mn, ma, mb = [m[k] for k in order]
    return [
        rho, mn, ma, mb, energy,
        mn * vn + p, ma * vn, mb * vn, (energy + p) * vn,
        root, vn, va, vb, c2, jnp.abs(vn) + sound,
    ]


FIRST, SECOND, THIRD = (0, 1, 2), (1, 0, 2), (2, 0, 1)


def put_cells(ref, row, arrays):
    for k, array in enumerate(arrays):
        ref[k, pl.ds(row, array.shape[0]), :] = array


def weno(d1, d2, d3, d4, eps):
    e1, e2, e3 = d2 - d1, d3 - d2, d4 - d3
    s2, s3 = 0.75 * d2, 0.75 * d3
    q2, q3 = s2 * d2 + eps, s3 * d3 + eps
    a = e1 * (e1 + s2) + q2
    b = e2 * (e2 + s2) + q2
    c = e3 * (e3 - s3) + q3
    bc, ac, ab = b * c, a * c, a * b
    w0 = bc * bc
    w1 = 6.0 * (ac * ac)
    w2 = 1.5 * (ab * ab)
    den = w0 + w1 + (w2 + w2)
    return (w0 * (e1 - e2) + w2 * (e2 - e3)) * rcp(den)


def face_tile(cells, flux, base, stride, row, rows=ROWS, step=None):
    def load(k, j):
        return cells[k, pl.ds(base + j * stride, rows, step), :]

    sl, sr = load(9, 2), load(9, 3)
    inv = rcp(sl + sr)
    wl, wr = sl * inv, sr * inv
    vl = [load(10 + k, 2) for k in range(3)]
    dv = [load(10 + k, 3) - vl[k] for k in range(3)]
    un, ta, tb = [vl[k] + wr * dv[k] for k in range(3)]
    jump = dv[0] * dv[0] + dv[1] * dv[1] + dv[2] * dv[2]
    c2 = wl * load(13, 2) + wr * load(13, 3) + (0.2 * (wl * wr)) * jump
    ic = lax.rsqrt(c2)
    sound = c2 * ic
    b1 = 0.4 * (ic * ic)
    qh = 0.5 * (un * un + ta * ta + tb * tb)
    enth = 2.5 * c2 + qh
    alpha = load(14, 0)
    for j in range(1, 6):
        alpha = jnp.maximum(alpha, load(14, j))

    state = [[load(k, j) for j in range(6)] for k in range(5)]
    phys = [state[1]] + [[load(k, j) for j in range(6)] for k in range(5, 9)]
    du = [[s[j + 1] - s[j] for j in range(5)] for s in state]
    df = [du[1]] + [[s[j + 1] - s[j] for j in range(5)] for s in phys[1:]]
    au = [[alpha * d for d in s] for s in du]

    def project(r, mn, ma, mb, e):
        s = (un * r - mn) * ic
        z = b1 * (e - un * mn - ta * ma - tb * mb + qh * r)
        return z + s, r - z, ma - ta * r, mb - tb * r, z - s

    plus = [project(*[df[k][j] + au[k][j] for k in range(5)]) for j in range(4)]
    minus = [project(*[df[k][j] - au[k][j] for k in range(5)]) for j in range(1, 5)]
    hats = []
    for k in range(5):
        eps = eps_outer if k in (0, 4) else eps_inner
        up = weno(plus[0][k], plus[1][k], plus[2][k], plus[3][k], eps)
        down = weno(minus[3][k], minus[2][k], minus[1][k], minus[0][k], eps)
        hats.append(up - down)
    lin = []
    for k in range(5):
        centre = 6.0 * (phys[k][2] + phys[k][3]) + (df[k][1] - df[k][3])
        lin.append(centre + ((au[k][1] + au[k][3]) - (au[k][2] + au[k][2])))
    h1, h2, h3, h4, h5 = hats
    h2, h3, h4 = h2 + h2, h3 + h3, h4 + h4
    h15 = h1 + h5
    k5 = sound * (h5 - h1)
    s = h15 + h2
    result = [
        lin[0] + s,
        lin[1] + (un * s + k5),
        lin[2] + (ta * s + h3),
        lin[3] + (tb * s + h4),
        lin[4] + (enth * h15 + un * k5 + qh * h2 + ta * h3 + tb * h4),
    ]
    for k in range(5):
        flux[k, pl.ds(row, rows, step), :] = result[k]


def is_star(counts):
    return math.prod(counts) <= 64 and counts[0] >= 4 and counts[1] >= 3 and counts[2] == 2


def kernel(
    counts, den_in, vel_in, pre_in, out,
    raw, cx, cy, cz, gx, gy, gz, acc, tz, hx, sy, hy, hz, top, got,
    in_sem, x_send, x_recv, y_send, y_recv, z_send, z_recv, top_send, top_recv, cast_send, cast_recv, permit,
):
    nx, ny, lanes = raw.shape[1:]
    nrow = nx * ny
    nz = lanes
    tiles = ny // ROWS
    ypad = ny + 2 * ROWS
    devices = math.prod(counts)
    star = is_star(counts)

    pairs = ((den_in, raw.at[0]), (vel_in, raw.at[pl.ds(1, 3)]), (pre_in, raw.at[4]))
    for a, b in pairs:
        pltpu.make_async_copy(a, b, in_sem).start()

    me = [lax.axis_index(a) for a in AXES]
    rank = (me[0] * counts[1] + me[1]) * counts[2] + me[2]
    roots = (0, counts[1] * counts[2])
    root = jnp.logical_and(me[0] <= 1, jnp.logical_and(me[1] == 0, me[2] == 0))
    odd = lax.rem(me[0], 2)
    last = me[1] == counts[1] - 1

    def device(d):
        return {
            "gx": lax.div(d, counts[1] * counts[2]),
            "gy": lax.rem(lax.div(d, counts[2]), counts[1]),
            "gz": lax.rem(d, counts[2]),
        }

    def near(axis, way):
        return {AXES[axis]: lax.rem(me[axis] + way + counts[axis], counts[axis])}

    barrier = pltpu.get_barrier_semaphore()

    def greet(peer):
        pl.semaphore_signal(barrier, inc=1, device_id=peer, device_id_type=MESH)

    ends = me[1] == 0, last
    lower = me[2] == 0
    if star:
        greet(near(0, 1))
        greet(near(0, -1))
        pl.when(jnp.logical_not(last))(lambda: greet(near(1, 1)))
        pl.when(ends[0])(lambda: greet(near(1, -1)))
        pl.when(lower)(lambda: greet(near(2, 1)))

        @pl.when(root)
        def _():
            @pl.loop(0, devices)
            def _(d):
                pl.when(d != rank)(lambda: greet(device(d)))

        greeted = 4 + jnp.where(ends[0], 0, 1) + jnp.where(last, 1, 0) + jnp.where(lower, 0, 1) - jnp.where(root, 1, 0)
    else:
        peers = [(a, {AXES[a]: lax.rem(me[a] + k, counts[a])}) for a in range(3) for k in range(1, counts[a])]
        greeted = len(peers)
        for _, peer in peers:
            greet(peer)

    pltpu.make_async_copy(raw, raw, in_sem).wait()

    def speeds(i, best):
        for t in range(tiles):
            r = t * ROWS
            inv_root = lax.rsqrt(raw[0, i, pl.ds(r, ROWS), :])
            c2 = gamma_gas * raw[4, i, pl.ds(r, ROWS), :] * (inv_root * inv_root)
            v1, v2, v3 = [jnp.abs(raw[1 + k, i, pl.ds(r, ROWS), :]) for k in range(3)]
            best = jnp.maximum(best, ((v1 + v2) + v3) + 3.0 * (c2 * lax.rsqrt(c2)))
        return best

    best = lax.fori_loop(0, nx, speeds, jnp.zeros((ROWS, lanes), jnp.float32))
    own = jnp.max(best, axis=0, keepdims=True)
    top[0] = own
    if star:
        got[rank] = own

    def own_cells():
        @pl.loop(0, nx)
        def _(i):
            for t in range(tiles):
                r = t * ROWS
                rho, v1, v2, v3, p = [raw[k, i, pl.ds(r, ROWS), :] for k in range(5)]
                basis = cell_basis(scale * rho, (v1, v2, v3), scale * p)
                put_cells(cx, pl.multiple_of((3 + i) * ny + r, ROWS), cell_arrays(basis, FIRST))
                put_cells(cy, pl.multiple_of(i * ypad + ROWS + r, ROWS), cell_arrays(basis, SECOND))

    def stage():
        for side, start in ((0, ny - 3), (1, 0)):
            for i in range(nx):
                for k in range(5):
                    sy[side, pl.ds(3 * (k * nx + i), 3), :] = raw[k, i, pl.ds(start, 3), :]
        for k in range(5):
            tz[k] = raw[k].reshape(nrow, nz).T

    def own_turned():
        @pl.loop(0, nz // ROWS, unroll=4)
        def _(t):
            r = pl.multiple_of(t * ROWS, ROWS)
            rho, v1, v2, v3, p = [tz[k, pl.ds(r, ROWS), :] for k in range(5)]
            basis = cell_basis(scale * rho, (v1, v2, v3), scale * p)
            put_cells(cz, r + ROWS, cell_arrays(basis, THIRD))

    def z_face(t):
        r = pl.multiple_of(t * ROWS, ROWS)
        face_tile(cz, gz, r + 5, 1, r)

    def y_face(i, t):
        face_tile(cy, gy, i * ypad + t * ROWS + 5, 1, pl.multiple_of(i * ypad + t * ROWS, ROWS))

    def pairs_of(body, start, number):
        @pl.loop(0, number // 2)
        def _(q):
            body(start + 2 * q)
            body(start + 2 * q + 1)

        if number % 2:
            body(start + number - 1)

    inside = nz // ROWS - 2
    first = 0
    if star:
        ahead = min(AHEAD, inside) // 2

        @pl.when(root)
        def _():
            stage()
            own_turned()
            pairs_of(z_face, 1, 2 * ahead)

        first = jnp.where(root, ahead, 0)

    pl.semaphore_wait(barrier, greeted)

    def remote(src, dst, send, recv, peer):
        return pltpu.make_async_remote_copy(
            src_ref=src, dst_ref=dst, send_sem=send, recv_sem=recv, device_id=peer, device_id_type=MESH
        )

    def to_root(k):
        return remote(top.at[0], got.at[rank], top_send, top_recv, device(jnp.int32(roots[k])))

    def cast(d):
        return remote(top.at[1], top.at[2], cast_send, cast_recv, device(jnp.int32(d)))

    def slots(number, send, recv):
        part = got.at[pl.ds(0, number)]
        return remote(part, part, send, recv, near(0, 1))

    def exchange(axis):
        return [
            remote(top.at[axis], got.at[slot], top_send.at[slot], top_recv.at[slot], peer)
            for slot, (other, peer) in enumerate(peers) if other == axis
        ]

    def next_top(axis):
        best = top[axis]
        for copy in exchange(axis):
            copy.wait()
        for slot, (other, _) in enumerate(peers):
            if other == axis:
                best = jnp.maximum(best, got[slot])
        top[axis + 1] = best
        if axis < 2:
            for copy in exchange(axis + 1):
                copy.start()

    def x_far(side, p):
        src = jnp.where(side == 0, nx - 1 - p, p)
        dst = jnp.where(side == 0, 2 - p, p)
        peer = near(0, jnp.where(side == 0, 1, -1))
        return remote(raw.at[:, src], hx.at[side, :, dst], x_send, x_recv.at[p], peer)

    def x_near(side):
        src = raw.at[:, pl.ds(jnp.where(side == 0, nx - 3, 0), 3)]
        return remote(src, hx.at[side], x_send, x_recv.at[3], near(0, jnp.where(side == 0, 1, -1)))

    def y_copy(side):
        return remote(sy.at[side], hy.at[side], y_send, y_recv.at[side], near(1, 1 - 2 * side))

    def z_copies():
        for side, start in ((0, nz - ROWS), (1, 0)):
            src = tz.at[:, pl.ds(start, ROWS), :]
            remote(src, hz.at[side], z_send, z_recv, near(2, 1 - 2 * side)).start()

    def allow(which, peer):
        pl.semaphore_signal(permit.at[which], inc=1, device_id=peer, device_id_type=MESH)

    if star:
        for k in range(2):
            pl.when(rank != roots[k])(lambda: to_root(k).start())
    else:
        for copy in exchange(0):
            copy.start()
    for p in range(3):
        x_far(1 - odd, p).start()
    x_near(odd).start()
    if star:
        pl.when(jnp.logical_not(ends[0]))(lambda: allow(0, near(1, -1)))
        pl.when(jnp.logical_not(lower))(lambda: allow(0, near(2, -1)))
        pl.when(last)(lambda: allow(1, near(1, 1)))

        @pl.when(jnp.logical_not(root))
        def _():
            stage()

        pl.when(last)(lambda: y_copy(0).start())
        pl.when(jnp.logical_not(ends[0]))(lambda: y_copy(1).start())
        pl.when(jnp.logical_not(lower))(z_copies)
        pl.when(jnp.logical_not(root))(own_turned)
    else:
        stage()
        z_copies()
        y_copy(0).start()
        y_copy(1).start()
        own_turned()
    own_cells()

    def z_pair(q, carry):
        z_face(1 + 2 * q)
        z_face(2 + 2 * q)
        return carry

    lax.fori_loop(first, inside // 2, z_pair, 0)
    if inside % 2:
        z_face(inside)
    if star:
        needed = jnp.where(last, 0, 1) + jnp.where(lower, 1, 0)
        pl.when(needed > 0)(lambda: pl.semaphore_wait(permit.at[0], needed))
        pl.when(lower)(z_copies)
        pl.when(jnp.logical_not(last))(lambda: y_copy(0).start())
    if not star:
        next_top(0)

    pairs_of(lambda q: y_face(q // (tiles - 2), lax.rem(q, tiles - 2) + 1), 0, nx * (tiles - 2))

    if not star:
        next_top(1)

    def x_plane(side, p):
        j = jnp.where(side == 0, 2 - p, p)
        base = jnp.where(side == 0, 2 - p, nx + 3 + p) * ny
        for t in range(tiles):
            r = t * ROWS
            rho, v1, v2, v3, pr = [hx[side, k, j, pl.ds(r, ROWS), :] for k in range(5)]
            basis = cell_basis(scale * rho, (v1, v2, v3), scale * pr)
            put_cells(cx, pl.multiple_of(base + r, ROWS), cell_arrays(basis, FIRST))

    def x_faces(start, number):
        def x_face(q):
            r = pl.multiple_of(start * ny + q * ROWS, ROWS)
            face_tile(cx, gx, r, ny, r)

        pairs_of(x_face, 0, number * tiles)

    x_near(1 - odd).wait_recv()
    pl.loop(0, 3)(lambda p: x_plane(1 - odd, p))
    x_faces(jnp.where(odd == 1, 0, 3), nx - 2)

    if star:
        @pl.when(ends[0])
        def _():
            pl.semaphore_wait(permit.at[1], 1)
            y_copy(1).start()

    remote(hz, hz, z_send, z_recv, near(2, 1)).wait_recv()
    for side, row in ((0, 0), (1, nz + ROWS)):
        rho, v1, v2, v3, p = [hz[side, k] for k in range(5)]
        put_cells(cz, row, cell_arrays(cell_basis(scale * rho, (v1, v2, v3), scale * p), THIRD))

    @pl.loop(0, 3)
    def _(t):
        z_face(jnp.where(t == 0, 0, nz // ROWS - 2 + t))

    for k, field in enumerate((0, 3, 1, 2, 4)):
        acc[field] = (gz[k, pl.ds(1, nz), :] - gz[k, pl.ds(0, nz), :]).T

    def y_side(side):
        y_copy(side).wait_recv()
        for i in range(nx):
            rho, v1, v2, v3, p = [hy[side, pl.ds(3 * (k * nx + i), 3), :] for k in range(5)]
            row = i * ypad + ROWS + (ny if side else -3)
            put_cells(cy, row, cell_arrays(cell_basis(scale * rho, (v1, v2, v3), scale * p), SECOND))

        pairs_of(lambda i: y_face(i, (tiles - 1) * side), 0, nx)

    def x_next(p):
        x_far(odd, p).wait_recv()
        x_plane(odd, p)
        x_faces(jnp.where(odd == 1, nx - 2 + p, 2 - p), 1)

    pl.when(last)(lambda: y_side(0))
    pl.when(jnp.logical_not(last))(lambda: y_side(1))
    pl.loop(0, 2)(x_next)
    pl.when(last)(lambda: y_side(1))
    pl.when(jnp.logical_not(last))(lambda: y_side(0))
    face_tile(cy, gy, ny + 5, 1, ny, nx, ypad)

    @pl.loop(0, nx)
    def _(i):
        for t in range(tiles):
            r = t * ROWS
            row = pl.multiple_of(i * ny + r, ROWS)
            yrow = pl.multiple_of(i * ypad + r, ROWS)
            for field, k in enumerate((0, 2, 1, 3, 4)):
                turn = gy[k, pl.ds(yrow + 1, ROWS), :] - gy[k, pl.ds(yrow, ROWS), :]
                acc[field, pl.ds(row, ROWS), :] = acc[field, pl.ds(row, ROWS), :] + turn

    def gather(k):
        @pl.when(rank == roots[k])
        def _():
            slots(devices - 1, top_send, top_recv).wait_recv()
            best = jnp.max(got[...], axis=0)
            top[1] = best
            top[2] = best
            if k == 1:
                for d in reversed(range(devices)):
                    if d not in roots:
                        cast(d).start()

    if star:
        gather(1)
    else:
        next_top(2)
    x_next(2)
    if star:
        gather(0)

    @pl.loop(0, nx)
    def _(i):
        for t in range(tiles):
            row = pl.multiple_of(i * ny + t * ROWS, ROWS)
            for field in range(5):
                turn = gx[field, pl.ds(row + ny, ROWS), :] - gx[field, pl.ds(row, ROWS), :]
                acc[field, pl.ds(row, ROWS), :] = acc[field, pl.ds(row, ROWS), :] + turn

    if star:
        pl.when(jnp.logical_not(root))(lambda: cast(0).wait_recv())
    largest = jnp.max(top[2 if star else 3], axis=(0, 1), keepdims=True)
    factor = jnp.broadcast_to((cfl_number / (12.0 * scale)) / largest, (ROWS, lanes))

    @pl.loop(0, nx)
    def _(i):
        for t in range(tiles):
            r = t * ROWS
            row = pl.multiple_of(i * ny + r, ROWS)
            for field in range(5):
                state = cx[field, pl.ds(pl.multiple_of(row + 3 * ny, ROWS), ROWS), :]
                out[field, i, pl.ds(r, ROWS), :] = (1.0 / scale) * state - factor * acc[field, pl.ds(row, ROWS), :]

    if star:
        pl.when(root)(lambda: slots(1, top_send, top_recv).wait_send())
        pl.when(jnp.logical_not(root))(lambda: slots(2, top_send, top_recv).wait_send())
        pl.when(rank == roots[1])(lambda: slots(devices - 2, cast_send, cast_recv).wait_send())
    remote(hx, hx, x_send, x_recv.at[0], near(0, 1)).wait_send()
    remote(sy, sy, y_send, y_recv.at[0], near(1, 1)).wait_send()
    remote(hz, hz, z_send, z_recv, near(2, 1)).wait_send()


def local(counts, density, velocity, pressure):
    nx, ny, nz = density.shape
    nrow = nx * ny
    slots = math.prod(counts) if is_star(counts) else sum(counts) - 3
    hands = [pltpu.SemaphoreType.DMA if is_star(counts) else pltpu.SemaphoreType.DMA((slots,))] * 2
    f32 = jnp.float32
    vmem = pl.BlockSpec(memory_space=pltpu.VMEM)
    edge = pl.cdiv(15 * nx, ROWS) * ROWS
    return pl.pallas_call(
        functools.partial(kernel, counts),
        out_shape=pltpu.VMEM((5, nx, ny, nz), f32),
        in_specs=[pl.BlockSpec(memory_space=pl.ANY)] * 3,
        out_specs=vmem,
        scratch_shapes=[
            pltpu.VMEM((5, nx, ny, nz), f32),
            pltpu.VMEM((15, (nx + 6) * ny + ROWS, nz), f32),
            pltpu.VMEM((15, nx * (ny + 2 * ROWS) + ROWS, nz), f32),
            pltpu.VMEM((15, nz + 3 * ROWS, nrow), f32),
            pltpu.VMEM((5, (nx + 1) * ny, nz), f32),
            pltpu.VMEM((5, nx * (ny + 2 * ROWS), nz), f32),
            pltpu.VMEM((5, nz + ROWS, nrow), f32),
            pltpu.VMEM((5, nrow, nz), f32),
            pltpu.VMEM((5, nz, nrow), f32),
            pltpu.VMEM((2, 5, 3, ny, nz), f32),
            pltpu.VMEM((2, edge, nz), f32),
            pltpu.VMEM((2, edge, nz), f32),
            pltpu.VMEM((2, 5, ROWS, nrow), f32),
            pltpu.VMEM((4, 1, nz), f32),
            pltpu.VMEM((slots, 1, nz), f32),
            pltpu.SemaphoreType.DMA,
            pltpu.SemaphoreType.DMA,
            pltpu.SemaphoreType.DMA((4,)),
            pltpu.SemaphoreType.DMA,
            pltpu.SemaphoreType.DMA((2,)),
            pltpu.SemaphoreType.DMA,
            pltpu.SemaphoreType.DMA,
            *hands,
            pltpu.SemaphoreType.DMA,
            pltpu.SemaphoreType.DMA,
            pltpu.SemaphoreType.REGULAR((2,)),
        ],
        compiler_params=pltpu.CompilerParams(collective_id=0, has_side_effects=True),
    )(density, velocity, pressure)


def solution(mesh):
    counts = tuple(mesh.shape[a] for a in AXES)
    in_specs = (P("gx", "gy", "gz"), P(None, "gx", "gy", "gz"), P("gx", "gy", "gz"))
    out_specs = P(None, "gx", "gy", "gz")
    return jax.shard_map(
        functools.partial(local, counts), mesh=mesh, in_specs=in_specs, out_specs=out_specs, check_vma=False
    )
```

```python
import functools
import math

import jax
import jax.numpy as jnp
from jax import lax
from jax.experimental import pallas as pl
from jax.experimental.pallas import tpu as pltpu
from jax.sharding import PartitionSpec as P

MESH = pl.DeviceIdType.MESH
AXES = ("gx", "gy", "gz")
gamma_gas = 1.4
weno_eps = 1e-06
cfl_number = 0.4
scale = 0.125
eps_outer = 0.75 * 16.0 * scale * scale * weno_eps
eps_inner = 0.75 * 4.0 * scale * scale * weno_eps
ROWS = 8
AHEAD = 8


def rcp(x):
    return pl.reciprocal(x)


def cell_basis(rho, v, p):
    inv_root = lax.rsqrt(rho)
    c2 = gamma_gas * p * (inv_root * inv_root)
    m = [rho * u for u in v]
    energy = 2.5 * p + 0.5 * (m[0] * v[0] + m[1] * v[1] + m[2] * v[2])
    return rho, v, p, m, energy, rho * inv_root, c2, c2 * lax.rsqrt(c2)


def cell_arrays(basis, order):
    rho, v, p, m, energy, root, c2, sound = basis
    vn, va, vb = [v[k] for k in order]
    mn, ma, mb = [m[k] for k in order]
    return [
        rho, mn, ma, mb, energy,
        mn * vn + p, ma * vn, mb * vn, (energy + p) * vn,
        root, vn, va, vb, c2, jnp.abs(vn) + sound,
    ]


FIRST, SECOND, THIRD = (0, 1, 2), (1, 0, 2), (2, 0, 1)


def put_cells(ref, row, arrays):
    for k, array in enumerate(arrays):
        ref[k, pl.ds(row, array.shape[0]), :] = array


def weno(d1, d2, d3, d4, eps):
    e1, e2, e3 = d2 - d1, d3 - d2, d4 - d3
    s2, s3 = 0.75 * d2, 0.75 * d3
    q2, q3 = s2 * d2 + eps, s3 * d3 + eps
    a = e1 * (e1 + s2) + q2
    b = e2 * (e2 + s2) + q2
    c = e3 * (e3 - s3) + q3
    bc, ac, ab = b * c, a * c, a * b
    w0 = bc * bc
    w1 = 6.0 * (ac * ac)
    w2 = 1.5 * (ab * ab)
    den = w0 + w1 + (w2 + w2)
    return (w0 * (e1 - e2) + w2 * (e2 - e3)) * rcp(den)


def face_tile(cells, flux, base, stride, row, rows=ROWS, step=None):
    def load(k, j):
        return cells[k, pl.ds(base + j * stride, rows, step), :]

    sl, sr = load(9, 2), load(9, 3)
    inv = rcp(sl + sr)
    wl, wr = sl * inv, sr * inv
    vl = [load(10 + k, 2) for k in range(3)]
    dv = [load(10 + k, 3) - vl[k] for k in range(3)]
    un, ta, tb = [vl[k] + wr * dv[k] for k in range(3)]
    jump = dv[0] * dv[0] + dv[1] * dv[1] + dv[2] * dv[2]
    c2 = wl * load(13, 2) + wr * load(13, 3) + (0.2 * (wl * wr)) * jump
    ic = lax.rsqrt(c2)
    sound = c2 * ic
    b1 = 0.4 * (ic * ic)
    qh = 0.5 * (un * un + ta * ta + tb * tb)
    enth = 2.5 * c2 + qh
    alpha = load(14, 0)
    for j in range(1, 6):
        alpha = jnp.maximum(alpha, load(14, j))

    state = [[load(k, j) for j in range(6)] for k in range(5)]
    phys = [state[1]] + [[load(k, j) for j in range(6)] for k in range(5, 9)]
    du = [[s[j + 1] - s[j] for j in range(5)] for s in state]
    df = [du[1]] + [[s[j + 1] - s[j] for j in range(5)] for s in phys[1:]]
    au = [[alpha * d for d in s] for s in du]

    def project(r, mn, ma, mb, e):
        s = (un * r - mn) * ic
        z = b1 * (e - un * mn - ta * ma - tb * mb + qh * r)
        return z + s, r - z, ma - ta * r, mb - tb * r, z - s

    plus = [project(*[df[k][j] + au[k][j] for k in range(5)]) for j in range(4)]
    minus = [project(*[df[k][j] - au[k][j] for k in range(5)]) for j in range(1, 5)]
    hats = []
    for k in range(5):
        eps = eps_outer if k in (0, 4) else eps_inner
        up = weno(plus[0][k], plus[1][k], plus[2][k], plus[3][k], eps)
        down = weno(minus[3][k], minus[2][k], minus[1][k], minus[0][k], eps)
        hats.append(up - down)
    lin = []
    for k in range(5):
        centre = 6.0 * (phys[k][2] + phys[k][3]) + (df[k][1] - df[k][3])
        lin.append(centre + ((au[k][1] + au[k][3]) - (au[k][2] + au[k][2])))
    h1, h2, h3, h4, h5 = hats
    h2, h3, h4 = h2 + h2, h3 + h3, h4 + h4
    h15 = h1 + h5
    k5 = sound * (h5 - h1)
    s = h15 + h2
    result = [
        lin[0] + s,
        lin[1] + (un * s + k5),
        lin[2] + (ta * s + h3),
        lin[3] + (tb * s + h4),
        lin[4] + (enth * h15 + un * k5 + qh * h2 + ta * h3 + tb * h4),
    ]
    for k in range(5):
        flux[k, pl.ds(row, rows, step), :] = result[k]


def is_star(counts):
    return math.prod(counts) <= 64 and counts[0] >= 4 and counts[1] >= 3 and counts[2] == 2


def kernel(
    counts, den_in, vel_in, pre_in, out,
    raw, cx, cy, cz, gx, gy, gz, acc, tz, hx, sy, hy, sz, hz, top, got,
    in_sem, x_send, x_recv, y_send, y_recv, z_send, z_recv, top_send, top_recv, cast_send, cast_recv, permit,
):
    nx, ny, lanes = raw.shape[1:]
    nrow = nx * ny
    nz = lanes
    tiles = ny // ROWS
    ypad = ny + 2 * ROWS
    half = ny // 2
    devices = math.prod(counts)
    star = is_star(counts)

    pairs = ((den_in, raw.at[0]), (vel_in, raw.at[pl.ds(1, 3)]), (pre_in, raw.at[4]))
    for a, b in pairs:
        pltpu.make_async_copy(a, b, in_sem).start()

    me = [lax.axis_index(a) for a in AXES]
    rank = (me[0] * counts[1] + me[1]) * counts[2] + me[2]
    roots = (0, counts[1] * counts[2])
    root = jnp.logical_and(me[0] <= 1, jnp.logical_and(me[1] == 0, me[2] == 0))
    odd = lax.rem(me[0], 2)
    last = me[1] == counts[1] - 1

    def device(d):
        return {
            "gx": lax.div(d, counts[1] * counts[2]),
            "gy": lax.rem(lax.div(d, counts[2]), counts[1]),
            "gz": lax.rem(d, counts[2]),
        }

    def near(axis, way):
        return {AXES[axis]: lax.rem(me[axis] + way + counts[axis], counts[axis])}

    barrier = pltpu.get_barrier_semaphore()

    def greet(peer):
        pl.semaphore_signal(barrier, inc=1, device_id=peer, device_id_type=MESH)

    ends = me[1] == 0, last
    lower = me[2] == 0
    if star:
        greet(near(0, 1))
        greet(near(0, -1))
        pl.when(jnp.logical_not(last))(lambda: greet(near(1, 1)))
        pl.when(ends[0])(lambda: greet(near(1, -1)))
        pl.when(lower)(lambda: greet(near(2, 1)))

        @pl.when(root)
        def _():
            @pl.loop(0, devices)
            def _(d):
                pl.when(d != rank)(lambda: greet(device(d)))

        greeted = 4 + jnp.where(ends[0], 0, 1) + jnp.where(last, 1, 0) + jnp.where(lower, 0, 1) - jnp.where(root, 1, 0)
    else:
        peers = [(a, {AXES[a]: lax.rem(me[a] + k, counts[a])}) for a in range(3) for k in range(1, counts[a])]
        greeted = len(peers)
        for _, peer in peers:
            greet(peer)

    pltpu.make_async_copy(raw, raw, in_sem).wait()

    def speeds(i, best):
        for t in range(tiles):
            r = t * ROWS
            inv_root = lax.rsqrt(raw[0, i, pl.ds(r, ROWS), :])
            c2 = gamma_gas * raw[4, i, pl.ds(r, ROWS), :] * (inv_root * inv_root)
            v1, v2, v3 = [jnp.abs(raw[1 + k, i, pl.ds(r, ROWS), :]) for k in range(3)]
            best = jnp.maximum(best, ((v1 + v2) + v3) + 3.0 * (c2 * lax.rsqrt(c2)))
        return best

    best = lax.fori_loop(0, nx, speeds, jnp.zeros((ROWS, lanes), jnp.float32))
    own = jnp.max(best, axis=0, keepdims=True)
    top[0] = own
    if star:
        got[rank] = own

    def own_cells():
        @pl.loop(0, nx)
        def _(i):
            for t in range(tiles):
                r = t * ROWS
                rho, v1, v2, v3, p = [raw[k, i, pl.ds(r, ROWS), :] for k in range(5)]
                basis = cell_basis(scale * rho, (v1, v2, v3), scale * p)
                put_cells(cx, pl.multiple_of((3 + i) * ny + r, ROWS), cell_arrays(basis, FIRST))
                put_cells(cy, pl.multiple_of(i * ypad + ROWS + r, ROWS), cell_arrays(basis, SECOND))

    def stage():
        for side, start in ((0, ny - 3), (1, 0)):
            for i in range(nx):
                for k in range(5):
                    sy[side, pl.ds(3 * (k * nx + i), 3), :] = raw[k, i, pl.ds(start, 3), :]
        for k in range(5):
            tz[k] = raw[k].reshape(nrow, nz).T
        for side, start in ((0, nz - 3), (1, 0)):
            for k in range(5):
                sz[side, pl.ds(3 * k, 3), :] = tz[k, pl.ds(start, 3), :]

    def own_turned():
        @pl.loop(0, nz // ROWS, unroll=4)
        def _(t):
            r = pl.multiple_of(t * ROWS, ROWS)
            rho, v1, v2, v3, p = [tz[k, pl.ds(r, ROWS), :] for k in range(5)]
            basis = cell_basis(scale * rho, (v1, v2, v3), scale * p)
            put_cells(cz, r + ROWS, cell_arrays(basis, THIRD))

    def z_face(t):
        r = pl.multiple_of(t * ROWS, ROWS)
        face_tile(cz, gz, r + 5, 1, r)

    def y_face(i, t):
        face_tile(cy, gy, i * ypad + t * ROWS + 5, 1, pl.multiple_of(i * ypad + t * ROWS, ROWS))

    def pairs_of(body, start, number):
        @pl.loop(0, number // 2)
        def _(q):
            body(start + 2 * q)
            body(start + 2 * q + 1)

        if number % 2:
            body(start + number - 1)

    inside = nz // ROWS - 2
    first = 0
    if star:
        ahead = min(AHEAD, inside) // 2

        @pl.when(root)
        def _():
            stage()
            own_turned()
            pairs_of(z_face, 1, 2 * ahead)

        first = jnp.where(root, ahead, 0)

    pl.semaphore_wait(barrier, greeted)

    def remote(src, dst, send, recv, peer):
        return pltpu.make_async_remote_copy(
            src_ref=src, dst_ref=dst, send_sem=send, recv_sem=recv, device_id=peer, device_id_type=MESH
        )

    def to_root(k):
        return remote(top.at[0], got.at[rank], top_send, top_recv, device(jnp.int32(roots[k])))

    def cast(d):
        return remote(top.at[1], top.at[2], cast_send, cast_recv, device(jnp.int32(d)))

    def slots(number, send, recv):
        part = got.at[pl.ds(0, number)]
        return remote(part, part, send, recv, near(0, 1))

    def exchange(axis):
        return [
            remote(top.at[axis], got.at[slot], top_send.at[slot], top_recv.at[slot], peer)
            for slot, (other, peer) in enumerate(peers) if other == axis
        ]

    def next_top(axis):
        best = top[axis]
        for copy in exchange(axis):
            copy.wait()
        for slot, (other, _) in enumerate(peers):
            if other == axis:
                best = jnp.maximum(best, got[slot])
        top[axis + 1] = best
        if axis < 2:
            for copy in exchange(axis + 1):
                copy.start()

    def x_far(side, p):
        src = jnp.where(side == 0, nx - 1 - p, p)
        dst = jnp.where(side == 0, 2 - p, p)
        peer = near(0, jnp.where(side == 0, 1, -1))
        return remote(raw.at[:, src], hx.at[side, :, dst], x_send, x_recv.at[p], peer)

    def x_half(side, h):
        src = jnp.where(side == 0, nx - 3, 2)
        dst = jnp.where(side == 0, 0, 2)
        rows = pl.ds(pl.multiple_of(h * half, ROWS), half)
        peer = near(0, jnp.where(side == 0, 1, -1))
        return remote(raw.at[:, src, rows], hx.at[side, :, dst, rows], x_send, x_recv.at[2 + h], peer)

    def x_near(side):
        src = raw.at[:, pl.ds(jnp.where(side == 0, nx - 3, 0), 3)]
        return remote(src, hx.at[side], x_send, x_recv.at[4], near(0, jnp.where(side == 0, 1, -1)))

    def y_copy(side):
        return remote(sy.at[side], hy.at[side], y_send, y_recv.at[side], near(1, 1 - 2 * side))

    def z_copies():
        for side in range(2):
            remote(sz.at[side], hz.at[side], z_send, z_recv, near(2, 1 - 2 * side)).start()

    def allow(which, peer):
        pl.semaphore_signal(permit.at[which], inc=1, device_id=peer, device_id_type=MESH)

    if star:
        for k in range(2):
            pl.when(rank != roots[k])(lambda: to_root(k).start())
    else:
        for copy in exchange(0):
            copy.start()
    for p in range(2):
        x_far(1 - odd, p).start()
    for h in range(2):
        x_half(1 - odd, h).start()
    x_near(odd).start()
    if star:
        pl.when(jnp.logical_not(ends[0]))(lambda: allow(0, near(1, -1)))
        pl.when(jnp.logical_not(lower))(lambda: allow(0, near(2, -1)))
        pl.when(last)(lambda: allow(1, near(1, 1)))

        @pl.when(jnp.logical_not(root))
        def _():
            stage()

        pl.when(last)(lambda: y_copy(0).start())
        pl.when(jnp.logical_not(ends[0]))(lambda: y_copy(1).start())
        pl.when(jnp.logical_not(lower))(z_copies)
        pl.when(jnp.logical_not(root))(own_turned)
    else:
        stage()
        z_copies()
        y_copy(0).start()
        y_copy(1).start()
        own_turned()
    own_cells()

    def z_pair(q, carry):
        z_face(1 + 2 * q)
        z_face(2 + 2 * q)
        return carry

    lax.fori_loop(first, inside // 2, z_pair, 0)
    if inside % 2:
        z_face(inside)
    pairs_of(lambda q: y_face(q // (tiles - 2), lax.rem(q, tiles - 2) + 1), 0, nx * (tiles - 2))

    def x_cells(side, p, start, rows):
        j = jnp.where(side == 0, 2 - p, p)
        base = jnp.where(side == 0, 2 - p, nx + 3 + p) * ny
        for t in range(rows // ROWS):
            r = pl.multiple_of(start + t * ROWS, ROWS)
            rho, v1, v2, v3, pr = [hx[side, k, j, pl.ds(r, ROWS), :] for k in range(5)]
            basis = cell_basis(scale * rho, (v1, v2, v3), scale * pr)
            put_cells(cx, pl.multiple_of(base + r, ROWS), cell_arrays(basis, FIRST))

    def x_faces(start, number):
        def x_face(q):
            r = pl.multiple_of(start + q * ROWS, ROWS)
            face_tile(cx, gx, r, ny, r)

        pairs_of(x_face, 0, number)

    if star:
        needed = jnp.where(last, 0, 1) + jnp.where(lower, 1, 0)
        pl.when(needed > 0)(lambda: pl.semaphore_wait(permit.at[0], needed))
        pl.when(lower)(z_copies)
        pl.when(jnp.logical_not(last))(lambda: y_copy(0).start())
    if not star:
        next_top(0)
        next_top(1)

    x_near(1 - odd).wait_recv()
    pl.loop(0, 3)(lambda p: x_cells(1 - odd, p, 0, ny))
    x_faces(jnp.where(odd == 1, 0, 3) * ny, (nx - 2) * tiles)

    if star:
        @pl.when(ends[0])
        def _():
            pl.semaphore_wait(permit.at[1], 1)
            y_copy(1).start()

    remote(hz, hz, z_send, z_recv, near(2, 1)).wait_recv()
    for side, row in ((0, ROWS - 3), (1, nz + ROWS)):
        rho, v1, v2, v3, p = [hz[side, pl.ds(3 * k, 3), :] for k in range(5)]
        put_cells(cz, row, cell_arrays(cell_basis(scale * rho, (v1, v2, v3), scale * p), THIRD))

    @pl.loop(0, 3)
    def _(t):
        z_face(jnp.where(t == 0, 0, nz // ROWS - 2 + t))

    for k, field in enumerate((0, 3, 1, 2, 4)):
        acc[field] = (gz[k, pl.ds(1, nz), :] - gz[k, pl.ds(0, nz), :]).T

    def y_side(side):
        y_copy(side).wait_recv()
        for i in range(nx):
            rho, v1, v2, v3, p = [hy[side, pl.ds(3 * (k * nx + i), 3), :] for k in range(5)]
            row = i * ypad + ROWS + (ny if side else -3)
            put_cells(cy, row, cell_arrays(cell_basis(scale * rho, (v1, v2, v3), scale * p), SECOND))

        pairs_of(lambda i: y_face(i, (tiles - 1) * side), 0, nx)

    def x_next(p):
        x_far(odd, p).wait_recv()
        x_cells(odd, p, 0, ny)
        x_faces(jnp.where(odd == 1, nx - 2 + p, 2 - p) * ny, tiles)

    def x_end(h):
        x_half(odd, h).wait_recv()
        x_cells(odd, 2, h * half, half)
        x_faces(jnp.where(odd == 1, nx, 0) * ny + h * half, half // ROWS)

    def set_factor(best):
        largest = jnp.max(best, axis=1, keepdims=True)
        top[4] = jnp.broadcast_to((cfl_number / (12.0 * scale)) / largest, (1, lanes))

    def gather(k):
        @pl.when(rank == roots[k])
        def _():
            slots(devices - 1, top_send, top_recv).wait_recv()
            best = jnp.max(got[...], axis=0)
            top[1] = best
            if k == 1:
                for d in reversed(range(devices)):
                    if d not in roots:
                        cast(d).start()
            set_factor(best)

    pl.when(last)(lambda: y_side(0))
    pl.when(jnp.logical_not(last))(lambda: y_side(1))
    turn = jnp.where(rank == roots[1], 1, 2) if star else 2

    def y_end():
        face_tile(cy, gy, ny + 5, 1, ny, nx, ypad)

    pl.when(jnp.logical_not(last))(y_end)

    def y_rest():
        @pl.when(last)
        def _():
            y_side(1)
            y_end()

        pl.when(jnp.logical_not(last))(lambda: y_side(0))

        @pl.loop(0, nx)
        def _(i):
            for t in range(tiles):
                r = t * ROWS
                row = pl.multiple_of(i * ny + r, ROWS)
                yrow = pl.multiple_of(i * ypad + r, ROWS)
                for field, k in enumerate((0, 2, 1, 3, 4)):
                    turn = gy[k, pl.ds(yrow + 1, ROWS), :] - gy[k, pl.ds(yrow, ROWS), :]
                    acc[field, pl.ds(row, ROWS), :] = acc[field, pl.ds(row, ROWS), :] + turn

    @pl.loop(0, 3)
    def _(p):
        pl.when(p == turn)(y_rest)
        if star:
            pl.when(p == 1)(lambda: gather(1))
        pl.when(p < 2)(lambda: x_next(p))

    pl.loop(0, 2)(x_end)

    @pl.loop(0, nx)
    def _(i):
        for t in range(tiles):
            row = pl.multiple_of(i * ny + t * ROWS, ROWS)
            for field in range(5):
                turn = gx[field, pl.ds(row + ny, ROWS), :] - gx[field, pl.ds(row, ROWS), :]
                acc[field, pl.ds(row, ROWS), :] = acc[field, pl.ds(row, ROWS), :] + turn

    if star:
        gather(0)

        @pl.when(jnp.logical_not(root))
        def _():
            cast(0).wait_recv()
            set_factor(top[2])
    else:
        next_top(2)
        set_factor(top[3])
    factor = jnp.broadcast_to(top[4], (ROWS, lanes))

    @pl.loop(0, nx)
    def _(i):
        for t in range(tiles):
            r = t * ROWS
            row = pl.multiple_of(i * ny + r, ROWS)
            for field in range(5):
                state = cx[field, pl.ds(pl.multiple_of(row + 3 * ny, ROWS), ROWS), :]
                out[field, i, pl.ds(r, ROWS), :] = (1.0 / scale) * state - factor * acc[field, pl.ds(row, ROWS), :]

    if star:
        pl.when(root)(lambda: slots(1, top_send, top_recv).wait_send())
        pl.when(jnp.logical_not(root))(lambda: slots(2, top_send, top_recv).wait_send())
        pl.when(rank == roots[1])(lambda: slots(devices - 2, cast_send, cast_recv).wait_send())
    remote(hx, hx, x_send, x_recv.at[0], near(0, 1)).wait_send()
    remote(sy, sy, y_send, y_recv.at[0], near(1, 1)).wait_send()
    remote(hz, hz, z_send, z_recv, near(2, 1)).wait_send()


def local(counts, density, velocity, pressure):
    nx, ny, nz = density.shape
    nrow = nx * ny
    slots = math.prod(counts) if is_star(counts) else sum(counts) - 3
    hands = [pltpu.SemaphoreType.DMA if is_star(counts) else pltpu.SemaphoreType.DMA((slots,))] * 2
    f32 = jnp.float32
    vmem = pl.BlockSpec(memory_space=pltpu.VMEM)
    edge = pl.cdiv(15 * nx, ROWS) * ROWS
    return pl.pallas_call(
        functools.partial(kernel, counts),
        out_shape=pltpu.VMEM((5, nx, ny, nz), f32),
        in_specs=[pl.BlockSpec(memory_space=pl.ANY)] * 3,
        out_specs=vmem,
        scratch_shapes=[
            pltpu.VMEM((5, nx, ny, nz), f32),
            pltpu.VMEM((15, (nx + 6) * ny + ROWS, nz), f32),
            pltpu.VMEM((15, nx * (ny + 2 * ROWS) + ROWS, nz), f32),
            pltpu.VMEM((15, nz + 3 * ROWS, nrow), f32),
            pltpu.VMEM((5, (nx + 1) * ny, nz), f32),
            pltpu.VMEM((5, nx * (ny + 2 * ROWS), nz), f32),
            pltpu.VMEM((5, nz + ROWS, nrow), f32),
            pltpu.VMEM((5, nrow, nz), f32),
            pltpu.VMEM((5, nz, nrow), f32),
            pltpu.VMEM((2, 5, 3, ny, nz), f32),
            pltpu.VMEM((2, edge, nz), f32),
            pltpu.VMEM((2, edge, nz), f32),
            pltpu.VMEM((2, 2 * ROWS, nrow), f32),
            pltpu.VMEM((2, 2 * ROWS, nrow), f32),
            pltpu.VMEM((5, 1, nz), f32),
            pltpu.VMEM((slots, 1, nz), f32),
            pltpu.SemaphoreType.DMA,
            pltpu.SemaphoreType.DMA,
            pltpu.SemaphoreType.DMA((5,)),
            pltpu.SemaphoreType.DMA,
            pltpu.SemaphoreType.DMA((2,)),
            pltpu.SemaphoreType.DMA,
            pltpu.SemaphoreType.DMA,
            *hands,
            pltpu.SemaphoreType.DMA,
            pltpu.SemaphoreType.DMA,
            pltpu.SemaphoreType.REGULAR((2,)),
        ],
        compiler_params=pltpu.CompilerParams(collective_id=0, has_side_effects=True),
    )(density, velocity, pressure)


def solution(mesh):
    counts = tuple(mesh.shape[a] for a in AXES)
    in_specs = (P("gx", "gy", "gz"), P(None, "gx", "gy", "gz"), P("gx", "gy", "gz"))
    out_specs = P(None, "gx", "gy", "gz")
    return jax.shard_map(
        functools.partial(local, counts), mesh=mesh, in_specs=in_specs, out_specs=out_specs, check_vma=False
    )
```

```python
import functools
import math

import jax
import jax.numpy as jnp
from jax import lax
from jax.experimental import pallas as pl
from jax.experimental.pallas import tpu as pltpu
from jax.sharding import PartitionSpec as P

MESH = pl.DeviceIdType.MESH
AXES = ("gx", "gy", "gz")
gamma_gas = 1.4
weno_eps = 1e-06
cfl_number = 0.4
scale = 0.125
eps_outer = 0.75 * 16.0 * scale * scale * weno_eps
eps_inner = 0.75 * 4.0 * scale * scale * weno_eps
ROWS = 8
AHEAD = 8


def rcp(x):
    return pl.reciprocal(x)


def cell_basis(rho, v, p):
    inv_root = lax.rsqrt(rho)
    c2 = gamma_gas * p * (inv_root * inv_root)
    m = [rho * u for u in v]
    energy = 2.5 * p + 0.5 * (m[0] * v[0] + m[1] * v[1] + m[2] * v[2])
    return rho, v, p, m, energy, rho * inv_root, c2, c2 * lax.rsqrt(c2)


def cell_arrays(basis, order):
    rho, v, p, m, energy, root, c2, sound = basis
    vn, va, vb = [v[k] for k in order]
    mn, ma, mb = [m[k] for k in order]
    return [
        rho, mn, ma, mb, energy,
        mn * vn + p, ma * vn, mb * vn, (energy + p) * vn,
        root, vn, va, vb, c2, jnp.abs(vn) + sound,
    ]


FIRST, SECOND, THIRD = (0, 1, 2), (1, 0, 2), (2, 0, 1)


def put_cells(ref, row, arrays):
    for k, array in enumerate(arrays):
        ref[k, pl.ds(row, array.shape[0]), :] = array


def weno(d1, d2, d3, d4, eps):
    e1, e2, e3 = d2 - d1, d3 - d2, d4 - d3
    s2, s3 = 0.75 * d2, 0.75 * d3
    q2, q3 = s2 * d2 + eps, s3 * d3 + eps
    a = e1 * (e1 + s2) + q2
    b = e2 * (e2 + s2) + q2
    c = e3 * (e3 - s3) + q3
    bc, ac, ab = b * c, a * c, a * b
    w0 = bc * bc
    w1 = 6.0 * (ac * ac)
    w2 = 1.5 * (ab * ab)
    den = w0 + w1 + (w2 + w2)
    return (w0 * (e1 - e2) + w2 * (e2 - e3)) * rcp(den)


def face_tile(cells, flux, base, stride, row, rows=ROWS, step=None):
    def load(k, j):
        return cells[k, pl.ds(base + j * stride, rows, step), :]

    sl, sr = load(9, 2), load(9, 3)
    inv = rcp(sl + sr)
    wl, wr = sl * inv, sr * inv
    vl = [load(10 + k, 2) for k in range(3)]
    dv = [load(10 + k, 3) - vl[k] for k in range(3)]
    un, ta, tb = [vl[k] + wr * dv[k] for k in range(3)]
    jump = dv[0] * dv[0] + dv[1] * dv[1] + dv[2] * dv[2]
    c2 = wl * load(13, 2) + wr * load(13, 3) + (0.2 * (wl * wr)) * jump
    ic = lax.rsqrt(c2)
    sound = c2 * ic
    b1 = 0.4 * (ic * ic)
    qh = 0.5 * (un * un + ta * ta + tb * tb)
    enth = 2.5 * c2 + qh
    alpha = load(14, 0)
    for j in range(1, 6):
        alpha = jnp.maximum(alpha, load(14, j))

    state = [[load(k, j) for j in range(6)] for k in range(5)]
    phys = [state[1]] + [[load(k, j) for j in range(6)] for k in range(5, 9)]
    du = [[s[j + 1] - s[j] for j in range(5)] for s in state]
    df = [du[1]] + [[s[j + 1] - s[j] for j in range(5)] for s in phys[1:]]
    au = [[alpha * d for d in s] for s in du]

    def project(r, mn, ma, mb, e):
        s = (un * r - mn) * ic
        z = b1 * (e - un * mn - ta * ma - tb * mb + qh * r)
        return z + s, r - z, ma - ta * r, mb - tb * r, z - s

    plus = [project(*[df[k][j] + au[k][j] for k in range(5)]) for j in range(4)]
    minus = [project(*[df[k][j] - au[k][j] for k in range(5)]) for j in range(1, 5)]
    hats = []
    for k in range(5):
        eps = eps_outer if k in (0, 4) else eps_inner
        up = weno(plus[0][k], plus[1][k], plus[2][k], plus[3][k], eps)
        down = weno(minus[3][k], minus[2][k], minus[1][k], minus[0][k], eps)
        hats.append(up - down)
    lin = []
    for k in range(5):
        centre = 6.0 * (phys[k][2] + phys[k][3]) + (df[k][1] - df[k][3])
        lin.append(centre + ((au[k][1] + au[k][3]) - (au[k][2] + au[k][2])))
    h1, h2, h3, h4, h5 = hats
    h2, h3, h4 = h2 + h2, h3 + h3, h4 + h4
    h15 = h1 + h5
    k5 = sound * (h5 - h1)
    s = h15 + h2
    result = [
        lin[0] + s,
        lin[1] + (un * s + k5),
        lin[2] + (ta * s + h3),
        lin[3] + (tb * s + h4),
        lin[4] + (enth * h15 + un * k5 + qh * h2 + ta * h3 + tb * h4),
    ]
    for k in range(5):
        flux[k, pl.ds(row, rows, step), :] = result[k]


def is_star(counts):
    return math.prod(counts) <= 64 and counts[0] >= 4 and counts[1] >= 3 and counts[2] == 2


def kernel(
    counts, den_in, vel_in, pre_in, out,
    raw, cx, cy, cz, gx, gy, gz, acc, tz, hx, sy, hy, sz, hz, top, got,
    x_send, x_recv, edge_send, y_recv, z_recv, top_send, top_recv, cast_recv, permit,
):
    nx, ny, lanes = raw.shape[1:]
    nrow = nx * ny
    nz = lanes
    tiles = ny // ROWS
    ypad = ny + 2 * ROWS
    half, quarter = ny // 2, ny // 4
    devices = math.prod(counts)
    star = is_star(counts)

    pairs = ((den_in, raw.at[0]), (vel_in, raw.at[pl.ds(1, 3)]), (pre_in, raw.at[4]))
    for a, b in pairs:
        pltpu.make_async_copy(a, b, x_send).start()

    me = [lax.axis_index(a) for a in AXES]
    rank = (me[0] * counts[1] + me[1]) * counts[2] + me[2]
    roots = (0, counts[1] * counts[2])
    root = jnp.logical_and(me[0] <= 1, jnp.logical_and(me[1] == 0, me[2] == 0))
    odd = lax.rem(me[0], 2)
    early = jnp.logical_or(root, me[0] == 1)
    last = me[1] == counts[1] - 1

    def device(d):
        return {
            "gx": lax.div(d, counts[1] * counts[2]),
            "gy": lax.rem(lax.div(d, counts[2]), counts[1]),
            "gz": lax.rem(d, counts[2]),
        }

    def near(axis, way):
        return {AXES[axis]: lax.rem(me[axis] + way + counts[axis], counts[axis])}

    barrier = pltpu.get_barrier_semaphore()

    def greet(peer):
        pl.semaphore_signal(barrier, inc=1, device_id=peer, device_id_type=MESH)

    ends = me[1] == 0, last
    lower = me[2] == 0
    if star:
        greet(near(0, 1))
        greet(near(0, -1))
        pl.when(jnp.logical_not(last))(lambda: greet(near(1, 1)))
        pl.when(ends[0])(lambda: greet(near(1, -1)))
        pl.when(lower)(lambda: greet(near(2, 1)))

        @pl.when(root)
        def _():
            @pl.loop(0, devices)
            def _(d):
                pl.when(d != rank)(lambda: greet(device(d)))

        greeted = 4 + jnp.where(ends[0], 0, 1) + jnp.where(last, 1, 0) + jnp.where(lower, 0, 1) - jnp.where(root, 1, 0)
    else:
        peers = [(a, {AXES[a]: lax.rem(me[a] + k, counts[a])}) for a in range(3) for k in range(1, counts[a])]
        greeted = len(peers)
        for _, peer in peers:
            greet(peer)

    pltpu.make_async_copy(raw, raw, x_send).wait()

    def speeds(i, best):
        for t in range(tiles):
            r = t * ROWS
            inv_root = lax.rsqrt(raw[0, i, pl.ds(r, ROWS), :])
            c2 = gamma_gas * raw[4, i, pl.ds(r, ROWS), :] * (inv_root * inv_root)
            v1, v2, v3 = [jnp.abs(raw[1 + k, i, pl.ds(r, ROWS), :]) for k in range(3)]
            best = jnp.maximum(best, ((v1 + v2) + v3) + 3.0 * (c2 * lax.rsqrt(c2)))
        return best

    best = lax.fori_loop(0, nx, speeds, jnp.zeros((ROWS, lanes), jnp.float32))
    own = jnp.max(best, axis=0, keepdims=True)
    top[0] = own
    if star:
        got[rank] = own
        top[1] = own

    def own_cells():
        @pl.loop(0, nx)
        def _(i):
            for t in range(tiles):
                r = t * ROWS
                rho, v1, v2, v3, p = [raw[k, i, pl.ds(r, ROWS), :] for k in range(5)]
                basis = cell_basis(scale * rho, (v1, v2, v3), scale * p)
                put_cells(cx, pl.multiple_of((3 + i) * ny + r, ROWS), cell_arrays(basis, FIRST))
                put_cells(cy, pl.multiple_of(i * ypad + ROWS + r, ROWS), cell_arrays(basis, SECOND))

    def stage_rows():
        for side, start in ((0, ny - 3), (1, 0)):
            for i in range(nx):
                for k in range(5):
                    sy[side, pl.ds(3 * (k * nx + i), 3), :] = raw[k, i, pl.ds(start, 3), :]

    def stage_turned():
        for k in range(5):
            tz[k] = raw[k].reshape(nrow, nz).T
        for side, start in ((0, nz - 3), (1, 0)):
            for k in range(5):
                sz[side, pl.ds(3 * k, 3), :] = tz[k, pl.ds(start, 3), :]

    def own_turned():
        @pl.loop(0, nz // ROWS, unroll=4)
        def _(t):
            r = pl.multiple_of(t * ROWS, ROWS)
            rho, v1, v2, v3, p = [tz[k, pl.ds(r, ROWS), :] for k in range(5)]
            basis = cell_basis(scale * rho, (v1, v2, v3), scale * p)
            put_cells(cz, r + ROWS, cell_arrays(basis, THIRD))

    def z_face(t):
        r = pl.multiple_of(t * ROWS, ROWS)
        face_tile(cz, gz, r + 5, 1, r)

    def y_face(i, t):
        face_tile(cy, gy, i * ypad + t * ROWS + 5, 1, pl.multiple_of(i * ypad + t * ROWS, ROWS))

    def pairs_of(body, start, number):
        @pl.loop(0, number // 2)
        def _(q):
            body(start + 2 * q)
            body(start + 2 * q + 1)

        if number % 2:
            body(start + number - 1)

    def z_pair(q, carry):
        z_face(1 + 2 * q)
        z_face(2 + 2 * q)
        return carry

    inside = nz // ROWS - 2
    first = 0
    if star:
        first = jnp.where(root, min(AHEAD, inside) // 2, jnp.where(early, 1, 0))

        @pl.when(early)
        def _():
            stage_rows()
            stage_turned()
            own_turned()
            lax.fori_loop(0, first, z_pair, 0)


    pl.semaphore_wait(barrier, greeted)

    def remote(src, dst, send, recv, peer):
        return pltpu.make_async_remote_copy(
            src_ref=src, dst_ref=dst, send_sem=send, recv_sem=recv, device_id=peer, device_id_type=MESH
        )

    def to_root(k):
        return remote(top.at[0], got.at[rank], top_send, top_recv, device(jnp.int32(roots[k])))

    def cast(d):
        return remote(top.at[1], top.at[2], top_send, cast_recv, device(jnp.int32(d)))

    def slots(number, send, recv):
        part = got.at[pl.ds(0, number)]
        return remote(part, part, send, recv, near(0, 1))

    def exchange(axis):
        return [
            remote(top.at[axis], got.at[slot], top_send.at[slot], top_recv.at[slot], peer)
            for slot, (other, peer) in enumerate(peers) if other == axis
        ]

    def next_top(axis):
        best = top[axis]
        for copy in exchange(axis):
            copy.wait()
        for slot, (other, _) in enumerate(peers):
            if other == axis:
                best = jnp.maximum(best, got[slot])
        top[axis + 1] = best
        if axis < 2:
            for copy in exchange(axis + 1):
                copy.start()

    def x_piece(side, p, start, rows, slot):
        src = jnp.where(side == 0, nx - 1 - p, p)
        dst = jnp.where(side == 0, 2 - p, p)
        part = pl.ds(pl.multiple_of(start, ROWS), rows)
        peer = near(0, jnp.where(side == 0, 1, -1))
        return remote(raw.at[:, src, part], hx.at[side, :, dst, part], x_send, x_recv.at[slot], peer)

    def x_half(side, q):
        return x_piece(side, lax.div(q, 2), lax.rem(q, 2) * half, half, q)

    def x_tail(side, q):
        return x_piece(side, 2, half + q * quarter, quarter, 5 + q)

    def x_near(side):
        src = raw.at[:, pl.ds(jnp.where(side == 0, nx - 3, 0), 3)]
        return remote(src, hx.at[side], x_send, x_recv.at[7], near(0, jnp.where(side == 0, 1, -1)))

    def y_copy(side):
        return remote(sy.at[side], hy.at[side], edge_send, y_recv.at[side], near(1, 1 - 2 * side))

    def z_copies():
        for side in range(2):
            remote(sz.at[side], hz.at[side], edge_send, z_recv, near(2, 1 - 2 * side)).start()

    def allow(which, peer):
        pl.semaphore_signal(permit.at[which], inc=1, device_id=peer, device_id_type=MESH)

    if star:
        for k in range(2):
            pl.when(rank != roots[k])(lambda: to_root(k).start())
    else:
        for copy in exchange(0):
            copy.start()
    for q in range(5):
        x_half(1 - odd, jnp.int32(q)).start()
    for q in range(2):
        x_tail(1 - odd, q).start()
    x_near(odd).start()
    if star:
        pl.when(jnp.logical_not(ends[0]))(lambda: allow(0, near(1, -1)))
        pl.when(jnp.logical_not(lower))(lambda: allow(0, near(2, -1)))
        pl.when(last)(lambda: allow(1, near(1, 1)))

        pl.when(jnp.logical_not(early))(stage_rows)
        pl.when(last)(lambda: y_copy(0).start())
        pl.when(jnp.logical_not(ends[0]))(lambda: y_copy(1).start())
        pl.when(jnp.logical_not(early))(stage_turned)
        pl.when(jnp.logical_not(lower))(z_copies)
        pl.when(jnp.logical_not(early))(own_turned)
    else:
        stage_rows()
        stage_turned()
        z_copies()
        y_copy(0).start()
        y_copy(1).start()
        own_turned()
    own_cells()

    lax.fori_loop(first, inside // 2, z_pair, 0)
    if inside % 2:
        z_face(inside)
    if star:
        needed = jnp.where(last, 0, 1) + jnp.where(lower, 1, 0)
        pl.when(needed > 0)(lambda: pl.semaphore_wait(permit.at[0], needed))
        pl.when(lower)(z_copies)
        pl.when(jnp.logical_not(last))(lambda: y_copy(0).start())
    pairs_of(lambda q: y_face(q // (tiles - 2), lax.rem(q, tiles - 2) + 1), 0, nx * (tiles - 2))

    def x_cells(side, p, start, rows):
        j = jnp.where(side == 0, 2 - p, p)
        base = jnp.where(side == 0, 2 - p, nx + 3 + p) * ny
        for t in range(rows // ROWS):
            r = pl.multiple_of(start + t * ROWS, ROWS)
            rho, v1, v2, v3, pr = [hx[side, k, j, pl.ds(r, ROWS), :] for k in range(5)]
            basis = cell_basis(scale * rho, (v1, v2, v3), scale * pr)
            put_cells(cx, pl.multiple_of(base + r, ROWS), cell_arrays(basis, FIRST))

    def x_faces(start, number):
        def x_face(q):
            r = pl.multiple_of(start + q * ROWS, ROWS)
            face_tile(cx, gx, r, ny, r)

        pairs_of(x_face, 0, number)

    if not star:
        next_top(0)
        next_top(1)

    x_near(1 - odd).wait_recv()
    pl.loop(0, 3)(lambda p: x_cells(1 - odd, p, 0, ny))
    x_faces(jnp.where(odd == 1, 0, 3) * ny, (nx - 2) * tiles)

    if star:
        @pl.when(ends[0])
        def _():
            pl.semaphore_wait(permit.at[1], 1)
            y_copy(1).start()

    remote(hz, hz, edge_send, z_recv, near(2, 1)).wait_recv()
    for side, row in ((0, ROWS - 3), (1, nz + ROWS)):
        rho, v1, v2, v3, p = [hz[side, pl.ds(3 * k, 3), :] for k in range(5)]
        put_cells(cz, row, cell_arrays(cell_basis(scale * rho, (v1, v2, v3), scale * p), THIRD))

    @pl.loop(0, 3)
    def _(t):
        z_face(jnp.where(t == 0, 0, nz // ROWS - 2 + t))

    for k, field in enumerate((0, 3, 1, 2, 4)):
        acc[field] = (gz[k, pl.ds(1, nz), :] - gz[k, pl.ds(0, nz), :]).T

    def y_side(side):
        y_copy(side).wait_recv()
        for i in range(nx):
            rho, v1, v2, v3, p = [hy[side, pl.ds(3 * (k * nx + i), 3), :] for k in range(5)]
            row = i * ypad + ROWS + (ny if side else -3)
            put_cells(cy, row, cell_arrays(cell_basis(scale * rho, (v1, v2, v3), scale * p), SECOND))

        pairs_of(lambda i: y_face(i, (tiles - 1) * side), 0, nx)

    def x_next(q):
        x_half(odd, q).wait_recv()
        p, start = lax.div(q, 2), lax.rem(q, 2) * half
        x_cells(odd, p, start, half)
        x_faces(jnp.where(odd == 1, nx - 2 + p, 2 - p) * ny + start, half // ROWS)

    def x_last(q):
        x_cells(odd, 2, half + q * quarter, quarter)
        x_faces(jnp.where(odd == 1, nx, 0) * ny + half + q * quarter, quarter // ROWS)

    def x_turn(i):
        for t in range(tiles):
            row = pl.multiple_of(i * ny + t * ROWS, ROWS)
            for field in range(5):
                turn = gx[field, pl.ds(row + ny, ROWS), :] - gx[field, pl.ds(row, ROWS), :]
                acc[field, pl.ds(row, ROWS), :] = acc[field, pl.ds(row, ROWS), :] + turn

    def set_factor(best):
        largest = jnp.max(best, axis=1, keepdims=True)
        top[4] = jnp.broadcast_to((cfl_number / (12.0 * scale)) / largest, (1, lanes))

    def gather(k):
        @pl.when(rank == roots[k])
        def _():
            slots(devices - 1, top_send, top_recv).wait_recv()
            best = jnp.max(got[...], axis=0)
            top[1] = best
            if k == 1:
                for d in reversed(range(devices)):
                    if d not in roots:
                        cast(d).start()

    pl.when(last)(lambda: y_side(0))
    pl.when(jnp.logical_not(last))(lambda: y_side(1))
    turn = jnp.where(rank == roots[1], 2, 4) if star else 4

    def y_end():
        face_tile(cy, gy, ny + 5, 1, ny, nx, ypad)

    pl.when(jnp.logical_not(last))(y_end)

    def y_rest():
        @pl.when(last)
        def _():
            y_side(1)
            y_end()

        pl.when(jnp.logical_not(last))(lambda: y_side(0))

        @pl.loop(0, nx)
        def _(i):
            for t in range(tiles):
                r = t * ROWS
                row = pl.multiple_of(i * ny + r, ROWS)
                yrow = pl.multiple_of(i * ypad + r, ROWS)
                for field, k in enumerate((0, 2, 1, 3, 4)):
                    turn = gy[k, pl.ds(yrow + 1, ROWS), :] - gy[k, pl.ds(yrow, ROWS), :]
                    acc[field, pl.ds(row, ROWS), :] = acc[field, pl.ds(row, ROWS), :] + turn

    @pl.loop(0, 5)
    def _(q):
        @pl.when(q == 4)
        def _():
            pl.loop(0, nx - 1)(lambda k: x_turn(k + 1 - odd))

        pl.when(q == turn)(y_rest)
        if star:
            pl.when(q == 3)(lambda: gather(1))
        x_next(q)

    x_tail(odd, 0).wait_recv()
    x_last(0)
    if star:
        gather(0)
    x_tail(odd, 1).wait_recv()
    if star:
        set_factor(top[1])
    x_last(1)
    x_turn(odd * (nx - 1))

    if star:
        @pl.when(jnp.logical_not(root))
        def _():
            cast(0).wait_recv()
            set_factor(top[2])
    else:
        next_top(2)
        set_factor(top[3])
    factor = jnp.broadcast_to(top[4], (ROWS, lanes))

    @pl.loop(0, nx)
    def _(i):
        for t in range(tiles):
            r = t * ROWS
            row = pl.multiple_of(i * ny + r, ROWS)
            for field in range(5):
                state = cx[field, pl.ds(pl.multiple_of(row + 3 * ny, ROWS), ROWS), :]
                out[field, i, pl.ds(r, ROWS), :] = (1.0 / scale) * state - factor * acc[field, pl.ds(row, ROWS), :]

    if star:
        pl.when(rank == roots[0])(lambda: slots(1, top_send, top_recv).wait_send())
        pl.when(rank == roots[1])(lambda: slots(devices - 1, top_send, top_recv).wait_send())
        pl.when(jnp.logical_not(root))(lambda: slots(2, top_send, top_recv).wait_send())
    remote(hx, hx, x_send, x_recv.at[0], near(0, 1)).wait_send()
    edges = cx.at[0, pl.ds(0, 2 * (sy.shape[1] + sz.shape[1]))]
    remote(edges, edges, edge_send, z_recv, near(2, 1)).wait_send()


def local(counts, density, velocity, pressure):
    nx, ny, nz = density.shape
    nrow = nx * ny
    slots = math.prod(counts) if is_star(counts) else sum(counts) - 3
    hands = [pltpu.SemaphoreType.DMA if is_star(counts) else pltpu.SemaphoreType.DMA((slots,))] * 2
    f32 = jnp.float32
    vmem = pl.BlockSpec(memory_space=pltpu.VMEM)
    edge = pl.cdiv(15 * nx, ROWS) * ROWS
    return pl.pallas_call(
        functools.partial(kernel, counts),
        out_shape=pltpu.VMEM((5, nx, ny, nz), f32),
        in_specs=[pl.BlockSpec(memory_space=pl.ANY)] * 3,
        out_specs=vmem,
        scratch_shapes=[
            pltpu.VMEM((5, nx, ny, nz), f32),
            pltpu.VMEM((15, (nx + 6) * ny + ROWS, nz), f32),
            pltpu.VMEM((15, nx * (ny + 2 * ROWS) + ROWS, nz), f32),
            pltpu.VMEM((15, nz + 3 * ROWS, nrow), f32),
            pltpu.VMEM((5, (nx + 1) * ny, nz), f32),
            pltpu.VMEM((5, nx * (ny + 2 * ROWS), nz), f32),
            pltpu.VMEM((5, nz + ROWS, nrow), f32),
            pltpu.VMEM((5, nrow, nz), f32),
            pltpu.VMEM((5, nz, nrow), f32),
            pltpu.VMEM((2, 5, 3, ny, nz), f32),
            pltpu.VMEM((2, edge, nz), f32),
            pltpu.VMEM((2, edge, nz), f32),
            pltpu.VMEM((2, 2 * ROWS, nrow), f32),
            pltpu.VMEM((2, 2 * ROWS, nrow), f32),
            pltpu.VMEM((5, 1, nz), f32),
            pltpu.VMEM((slots, 1, nz), f32),
            pltpu.SemaphoreType.DMA,
            pltpu.SemaphoreType.DMA((8,)),
            pltpu.SemaphoreType.DMA,
            pltpu.SemaphoreType.DMA((2,)),
            pltpu.SemaphoreType.DMA,
            *hands,
            pltpu.SemaphoreType.DMA,
            pltpu.SemaphoreType.REGULAR((2,)),
        ],
        compiler_params=pltpu.CompilerParams(collective_id=0, has_side_effects=True),
    )(density, velocity, pressure)


def solution(mesh):
    counts = tuple(mesh.shape[a] for a in AXES)
    in_specs = (P("gx", "gy", "gz"), P(None, "gx", "gy", "gz"), P("gx", "gy", "gz"))
    out_specs = P(None, "gx", "gy", "gz")
    return jax.shard_map(
        functools.partial(local, counts), mesh=mesh, in_specs=in_specs, out_specs=out_specs, check_vma=False
    )
```

```python
import functools
import math

import jax
import jax.numpy as jnp
from jax import lax
from jax.experimental import pallas as pl
from jax.experimental.pallas import tpu as pltpu
from jax.sharding import PartitionSpec as P

MESH = pl.DeviceIdType.MESH
AXES = ("gx", "gy", "gz")
gamma_gas = 1.4
weno_eps = 1e-06
cfl_number = 0.4
scale = 0.125
eps_outer = 0.75 * 16.0 * scale * scale * weno_eps
eps_inner = 0.75 * 4.0 * scale * scale * weno_eps
ROWS = 8
AHEAD = 8


def rcp(x):
    return pl.reciprocal(x)


def cell_basis(rho, v, p):
    inv_root = lax.rsqrt(rho)
    c2 = gamma_gas * p * (inv_root * inv_root)
    m = [rho * u for u in v]
    energy = 2.5 * p + 0.5 * (m[0] * v[0] + m[1] * v[1] + m[2] * v[2])
    return rho, v, p, m, energy, rho * inv_root, c2, c2 * lax.rsqrt(c2)


def cell_arrays(basis, order):
    rho, v, p, m, energy, root, c2, sound = basis
    vn, va, vb = [v[k] for k in order]
    mn, ma, mb = [m[k] for k in order]
    return [
        rho, mn, ma, mb, energy,
        mn * vn + p, ma * vn, mb * vn, (energy + p) * vn,
        root, vn, va, vb, c2, jnp.abs(vn) + sound,
    ]


FIRST, SECOND, THIRD = (0, 1, 2), (1, 0, 2), (2, 0, 1)


def put_cells(ref, row, arrays):
    for k, array in enumerate(arrays):
        ref[k, pl.ds(row, array.shape[0]), :] = array


def weno(d1, d2, d3, d4, eps):
    e1, e2, e3 = d2 - d1, d3 - d2, d4 - d3
    s2, s3 = 0.75 * d2, 0.75 * d3
    q2, q3 = s2 * d2 + eps, s3 * d3 + eps
    a = e1 * (e1 + s2) + q2
    b = e2 * (e2 + s2) + q2
    c = e3 * (e3 - s3) + q3
    bc, ac, ab = b * c, a * c, a * b
    w0 = bc * bc
    w1 = 6.0 * (ac * ac)
    w2 = 1.5 * (ab * ab)
    den = w0 + w1 + (w2 + w2)
    return (w0 * (e1 - e2) + w2 * (e2 - e3)) * rcp(den)


def face_tile(cells, flux, base, stride, row, rows=ROWS, step=None):
    def load(k, j):
        return cells[k, pl.ds(base + j * stride, rows, step), :]

    sl, sr = load(9, 2), load(9, 3)
    inv = rcp(sl + sr)
    wl, wr = sl * inv, sr * inv
    vl = [load(10 + k, 2) for k in range(3)]
    dv = [load(10 + k, 3) - vl[k] for k in range(3)]
    un, ta, tb = [vl[k] + wr * dv[k] for k in range(3)]
    jump = dv[0] * dv[0] + dv[1] * dv[1] + dv[2] * dv[2]
    c2 = wl * load(13, 2) + wr * load(13, 3) + (0.2 * (wl * wr)) * jump
    ic = lax.rsqrt(c2)
    sound = c2 * ic
    b1 = 0.4 * (ic * ic)
    qh = 0.5 * (un * un + ta * ta + tb * tb)
    enth = 2.5 * c2 + qh
    alpha = load(14, 0)
    for j in range(1, 6):
        alpha = jnp.maximum(alpha, load(14, j))

    state = [[load(k, j) for j in range(6)] for k in range(5)]
    phys = [state[1]] + [[load(k, j) for j in range(6)] for k in range(5, 9)]
    du = [[s[j + 1] - s[j] for j in range(5)] for s in state]
    df = [du[1]] + [[s[j + 1] - s[j] for j in range(5)] for s in phys[1:]]
    au = [[alpha * d for d in s] for s in du]

    def project(r, mn, ma, mb, e):
        s = (un * r - mn) * ic
        z = b1 * (e - un * mn - ta * ma - tb * mb + qh * r)
        return z + s, r - z, ma - ta * r, mb - tb * r, z - s

    plus = [project(*[df[k][j] + au[k][j] for k in range(5)]) for j in range(4)]
    minus = [project(*[df[k][j] - au[k][j] for k in range(5)]) for j in range(1, 5)]
    hats = []
    for k in range(5):
        eps = eps_outer if k in (0, 4) else eps_inner
        up = weno(plus[0][k], plus[1][k], plus[2][k], plus[3][k], eps)
        down = weno(minus[3][k], minus[2][k], minus[1][k], minus[0][k], eps)
        hats.append(up - down)
    lin = []
    for k in range(5):
        centre = 6.0 * (phys[k][2] + phys[k][3]) + (df[k][1] - df[k][3])
        lin.append(centre + ((au[k][1] + au[k][3]) - (au[k][2] + au[k][2])))
    h1, h2, h3, h4, h5 = hats
    h2, h3, h4 = h2 + h2, h3 + h3, h4 + h4
    h15 = h1 + h5
    k5 = sound * (h5 - h1)
    s = h15 + h2
    result = [
        lin[0] + s,
        lin[1] + (un * s + k5),
        lin[2] + (ta * s + h3),
        lin[3] + (tb * s + h4),
        lin[4] + (enth * h15 + un * k5 + qh * h2 + ta * h3 + tb * h4),
    ]
    for k in range(5):
        flux[k, pl.ds(row, rows, step), :] = result[k]


def is_star(counts):
    return math.prod(counts) <= 64 and counts[0] >= 4 and counts[1] >= 3 and counts[2] == 2


def kernel(
    counts, den_in, vel_in, pre_in, out,
    raw, cx, cy, cz, gx, gy, gz, acc, tz, hx, sy, hy, sz, hz, top, got,
    x_send, x_recv, edge_send, y_recv, z_recv, top_send, top_recv, cast_recv, permit,
):
    nx, ny, lanes = raw.shape[1:]
    nrow = nx * ny
    nz = lanes
    tiles = ny // ROWS
    ypad = ny + 2 * ROWS
    half, quarter = ny // 2, ny // 4
    devices = math.prod(counts)
    star = is_star(counts)

    for i in range(0, nx, 1):
        part = pl.ds(i, 1)
        pltpu.make_async_copy(den_in.at[part], raw.at[0, part], x_send).start()
        for k in range(3):
            pltpu.make_async_copy(vel_in.at[k, part], raw.at[1 + k, part], x_send).start()
        pltpu.make_async_copy(pre_in.at[part], raw.at[4, part], x_send).start()

    me = [lax.axis_index(a) for a in AXES]
    rank = (me[0] * counts[1] + me[1]) * counts[2] + me[2]
    roots = (0, counts[1] * counts[2])
    root = jnp.logical_and(me[0] <= 1, jnp.logical_and(me[1] == 0, me[2] == 0))
    odd = lax.rem(me[0], 2)
    early = jnp.logical_or(root, me[0] == 1)
    last = me[1] == counts[1] - 1

    def device(d):
        return {
            "gx": lax.div(d, counts[1] * counts[2]),
            "gy": lax.rem(lax.div(d, counts[2]), counts[1]),
            "gz": lax.rem(d, counts[2]),
        }

    def near(axis, way):
        return {AXES[axis]: lax.rem(me[axis] + way + counts[axis], counts[axis])}

    barrier = pltpu.get_barrier_semaphore()

    def greet(peer):
        pl.semaphore_signal(barrier, inc=1, device_id=peer, device_id_type=MESH)

    ends = me[1] == 0, last
    lower = me[2] == 0
    if star:
        greet(near(0, 1))
        greet(near(0, -1))
        pl.when(jnp.logical_not(last))(lambda: greet(near(1, 1)))
        pl.when(ends[0])(lambda: greet(near(1, -1)))
        pl.when(lower)(lambda: greet(near(2, 1)))

        @pl.when(root)
        def _():
            @pl.loop(0, devices)
            def _(d):
                pl.when(d != rank)(lambda: greet(device(d)))

        greeted = 4 + jnp.where(ends[0], 0, 1) + jnp.where(last, 1, 0) + jnp.where(lower, 0, 1) - jnp.where(root, 1, 0)
    else:
        peers = [(a, {AXES[a]: lax.rem(me[a] + k, counts[a])}) for a in range(3) for k in range(1, counts[a])]
        greeted = len(peers)
        for _, peer in peers:
            greet(peer)

    pltpu.make_async_copy(raw, raw, x_send).wait()

    def speeds(i, best):
        for t in range(tiles):
            r = t * ROWS
            inv_root = lax.rsqrt(raw[0, i, pl.ds(r, ROWS), :])
            c2 = gamma_gas * raw[4, i, pl.ds(r, ROWS), :] * (inv_root * inv_root)
            v1, v2, v3 = [jnp.abs(raw[1 + k, i, pl.ds(r, ROWS), :]) for k in range(3)]
            best = jnp.maximum(best, ((v1 + v2) + v3) + 3.0 * (c2 * lax.rsqrt(c2)))
        return best

    best = lax.fori_loop(0, nx, speeds, jnp.zeros((ROWS, lanes), jnp.float32))
    own = jnp.max(best, axis=0, keepdims=True)
    top[0] = own
    if star:
        got[rank] = own
        top[1] = own

    def own_cells():
        @pl.loop(0, nx)
        def _(i):
            for t in range(tiles):
                r = t * ROWS
                rho, v1, v2, v3, p = [raw[k, i, pl.ds(r, ROWS), :] for k in range(5)]
                basis = cell_basis(scale * rho, (v1, v2, v3), scale * p)
                put_cells(cx, pl.multiple_of((3 + i) * ny + r, ROWS), cell_arrays(basis, FIRST))
                put_cells(cy, pl.multiple_of(i * ypad + ROWS + r, ROWS), cell_arrays(basis, SECOND))

    def stage_rows():
        for side, start in ((0, ny - 3), (1, 0)):
            for i in range(nx):
                for k in range(5):
                    sy[side, pl.ds(3 * (k * nx + i), 3), :] = raw[k, i, pl.ds(start, 3), :]

    def stage_turned():
        for k in range(5):
            tz[k] = raw[k].reshape(nrow, nz).T
        for side, start in ((0, nz - 3), (1, 0)):
            for k in range(5):
                sz[side, pl.ds(3 * k, 3), :] = tz[k, pl.ds(start, 3), :]

    def own_turned():
        @pl.loop(0, nz // ROWS, unroll=4)
        def _(t):
            r = pl.multiple_of(t * ROWS, ROWS)
            rho, v1, v2, v3, p = [tz[k, pl.ds(r, ROWS), :] for k in range(5)]
            basis = cell_basis(scale * rho, (v1, v2, v3), scale * p)
            put_cells(cz, r + ROWS, cell_arrays(basis, THIRD))

    def z_face(t):
        r = pl.multiple_of(t * ROWS, ROWS)
        face_tile(cz, gz, r + 5, 1, r)

    def y_face(i, t):
        face_tile(cy, gy, i * ypad + t * ROWS + 5, 1, pl.multiple_of(i * ypad + t * ROWS, ROWS))

    def pairs_of(body, start, number):
        @pl.loop(0, number // 2)
        def _(q):
            body(start + 2 * q)
            body(start + 2 * q + 1)

        if number % 2:
            body(start + number - 1)

    def z_pair(q, carry):
        z_face(1 + 2 * q)
        z_face(2 + 2 * q)
        return carry

    inside = nz // ROWS - 2
    first = 0
    if star:
        first = jnp.where(root, min(AHEAD, inside) // 2, jnp.where(early, 1, 0))

        @pl.when(early)
        def _():
            stage_rows()
            stage_turned()
            own_turned()
            lax.fori_loop(0, first, z_pair, 0)


    pl.semaphore_wait(barrier, greeted)

    def remote(src, dst, send, recv, peer):
        return pltpu.make_async_remote_copy(
            src_ref=src, dst_ref=dst, send_sem=send, recv_sem=recv, device_id=peer, device_id_type=MESH
        )

    def to_root(k):
        return remote(top.at[0], got.at[rank], top_send, top_recv, device(jnp.int32(roots[k])))

    def cast(d):
        return remote(top.at[1], top.at[2], top_send, cast_recv, device(jnp.int32(d)))

    def slots(number, send, recv):
        part = got.at[pl.ds(0, number)]
        return remote(part, part, send, recv, near(0, 1))

    def exchange(axis):
        return [
            remote(top.at[axis], got.at[slot], top_send.at[slot], top_recv.at[slot], peer)
            for slot, (other, peer) in enumerate(peers) if other == axis
        ]

    def next_top(axis):
        best = top[axis]
        for copy in exchange(axis):
            copy.wait()
        for slot, (other, _) in enumerate(peers):
            if other == axis:
                best = jnp.maximum(best, got[slot])
        top[axis + 1] = best
        if axis < 2:
            for copy in exchange(axis + 1):
                copy.start()

    def x_piece(side, p, start, rows, slot):
        src = jnp.where(side == 0, nx - 1 - p, p)
        dst = jnp.where(side == 0, 2 - p, p)
        part = pl.ds(pl.multiple_of(start, ROWS), rows)
        peer = near(0, jnp.where(side == 0, 1, -1))
        return remote(raw.at[:, src, part], hx.at[side, :, dst, part], x_send, x_recv.at[slot], peer)

    def x_half(side, q):
        return x_piece(side, lax.div(q, 2), lax.rem(q, 2) * half, half, q)

    def x_tail(side, q):
        return x_piece(side, 2, half + q * quarter, quarter, 5 + q)

    def x_near(side):
        src = raw.at[:, pl.ds(jnp.where(side == 0, nx - 3, 0), 3)]
        return remote(src, hx.at[side], x_send, x_recv.at[7], near(0, jnp.where(side == 0, 1, -1)))

    def y_copy(side):
        return remote(sy.at[side], hy.at[side], edge_send, y_recv.at[side], near(1, 1 - 2 * side))

    def z_copies():
        for side in range(2):
            remote(sz.at[side], hz.at[side], edge_send, z_recv, near(2, 1 - 2 * side)).start()

    def allow(which, peer):
        pl.semaphore_signal(permit.at[which], inc=1, device_id=peer, device_id_type=MESH)

    if star:
        for k in range(2):
            pl.when(rank != roots[k])(lambda: to_root(k).start())
    else:
        for copy in exchange(0):
            copy.start()
    for q in range(5):
        x_half(1 - odd, jnp.int32(q)).start()
    for q in range(2):
        x_tail(1 - odd, q).start()
    x_near(odd).start()
    if star:
        pl.when(jnp.logical_not(ends[0]))(lambda: allow(0, near(1, -1)))
        pl.when(jnp.logical_not(lower))(lambda: allow(0, near(2, -1)))
        pl.when(last)(lambda: allow(1, near(1, 1)))

        pl.when(jnp.logical_not(early))(stage_rows)
        pl.when(last)(lambda: y_copy(0).start())
        pl.when(jnp.logical_not(ends[0]))(lambda: y_copy(1).start())
        pl.when(jnp.logical_not(early))(stage_turned)
        pl.when(jnp.logical_not(lower))(z_copies)
        pl.when(jnp.logical_not(early))(own_turned)
    else:
        stage_rows()
        stage_turned()
        z_copies()
        y_copy(0).start()
        y_copy(1).start()
        own_turned()
    own_cells()

    lax.fori_loop(first, inside // 2, z_pair, 0)
    if inside % 2:
        z_face(inside)
    if star:
        needed = jnp.where(last, 0, 1) + jnp.where(lower, 1, 0)
        pl.when(needed > 0)(lambda: pl.semaphore_wait(permit.at[0], needed))
        pl.when(lower)(z_copies)
        pl.when(jnp.logical_not(last))(lambda: y_copy(0).start())
    pairs_of(lambda q: y_face(q // (tiles - 2), lax.rem(q, tiles - 2) + 1), 0, nx * (tiles - 2))

    def x_cells(side, p, start, rows):
        j = jnp.where(side == 0, 2 - p, p)
        base = jnp.where(side == 0, 2 - p, nx + 3 + p) * ny
        for t in range(rows // ROWS):
            r = pl.multiple_of(start + t * ROWS, ROWS)
            rho, v1, v2, v3, pr = [hx[side, k, j, pl.ds(r, ROWS), :] for k in range(5)]
            basis = cell_basis(scale * rho, (v1, v2, v3), scale * pr)
            put_cells(cx, pl.multiple_of(base + r, ROWS), cell_arrays(basis, FIRST))

    def x_faces(start, number):
        def x_face(q):
            r = pl.multiple_of(start + q * ROWS, ROWS)
            face_tile(cx, gx, r, ny, r)

        pairs_of(x_face, 0, number)

    if not star:
        next_top(0)
        next_top(1)

    x_near(1 - odd).wait_recv()
    pl.loop(0, 3)(lambda p: x_cells(1 - odd, p, 0, ny))
    x_faces(jnp.where(odd == 1, 0, 3) * ny, (nx - 2) * tiles)

    if star:
        @pl.when(ends[0])
        def _():
            pl.semaphore_wait(permit.at[1], 1)
            y_copy(1).start()

    remote(hz, hz, edge_send, z_recv, near(2, 1)).wait_recv()
    for side, row in ((0, ROWS - 3), (1, nz + ROWS)):
        rho, v1, v2, v3, p = [hz[side, pl.ds(3 * k, 3), :] for k in range(5)]
        put_cells(cz, row, cell_arrays(cell_basis(scale * rho, (v1, v2, v3), scale * p), THIRD))

    @pl.loop(0, 3)
    def _(t):
        z_face(jnp.where(t == 0, 0, nz // ROWS - 2 + t))

    for k, field in enumerate((0, 3, 1, 2, 4)):
        acc[field] = (gz[k, pl.ds(1, nz), :] - gz[k, pl.ds(0, nz), :]).T

    def y_side(side):
        y_copy(side).wait_recv()
        for i in range(nx):
            rho, v1, v2, v3, p = [hy[side, pl.ds(3 * (k * nx + i), 3), :] for k in range(5)]
            row = i * ypad + ROWS + (ny if side else -3)
            put_cells(cy, row, cell_arrays(cell_basis(scale * rho, (v1, v2, v3), scale * p), SECOND))

        pairs_of(lambda i: y_face(i, (tiles - 1) * side), 0, nx)

    def x_next(q):
        x_half(odd, q).wait_recv()
        p, start = lax.div(q, 2), lax.rem(q, 2) * half
        x_cells(odd, p, start, half)
        x_faces(jnp.where(odd == 1, nx - 2 + p, 2 - p) * ny + start, half // ROWS)

    def x_last(q):
        x_cells(odd, 2, half + q * quarter, quarter)
        x_faces(jnp.where(odd == 1, nx, 0) * ny + half + q * quarter, quarter // ROWS)

    def x_turn(i):
        for t in range(tiles):
            row = pl.multiple_of(i * ny + t * ROWS, ROWS)
            for field in range(5):
                turn = gx[field, pl.ds(row + ny, ROWS), :] - gx[field, pl.ds(row, ROWS), :]
                acc[field, pl.ds(row, ROWS), :] = acc[field, pl.ds(row, ROWS), :] + turn

    def set_factor(best):
        largest = jnp.max(best, axis=1, keepdims=True)
        top[4] = jnp.broadcast_to((cfl_number / (12.0 * scale)) / largest, (1, lanes))

    def gather(k):
        @pl.when(rank == roots[k])
        def _():
            slots(devices - 1, top_send, top_recv).wait_recv()
            best = jnp.max(got[...], axis=0)
            top[1] = best
            if k == 1:
                for d in reversed(range(devices)):
                    if d not in roots:
                        cast(d).start()

    pl.when(last)(lambda: y_side(0))
    pl.when(jnp.logical_not(last))(lambda: y_side(1))
    turn = jnp.where(rank == roots[1], 2, 4) if star else 4

    def y_end():
        face_tile(cy, gy, ny + 5, 1, ny, nx, ypad)

    pl.when(jnp.logical_not(last))(y_end)

    def y_rest():
        @pl.when(last)
        def _():
            y_side(1)
            y_end()

        pl.when(jnp.logical_not(last))(lambda: y_side(0))

        @pl.loop(0, nx)
        def _(i):
            for t in range(tiles):
                r = t * ROWS
                row = pl.multiple_of(i * ny + r, ROWS)
                yrow = pl.multiple_of(i * ypad + r, ROWS)
                for field, k in enumerate((0, 2, 1, 3, 4)):
                    turn = gy[k, pl.ds(yrow + 1, ROWS), :] - gy[k, pl.ds(yrow, ROWS), :]
                    acc[field, pl.ds(row, ROWS), :] = acc[field, pl.ds(row, ROWS), :] + turn

    @pl.loop(0, 5)
    def _(q):
        @pl.when(q == 4)
        def _():
            pl.loop(0, nx - 1)(lambda k: x_turn(k + 1 - odd))

        pl.when(q == turn)(y_rest)
        if star:
            pl.when(q == 3)(lambda: gather(1))
        x_next(q)

    x_tail(odd, 0).wait_recv()
    x_last(0)
    if star:
        gather(0)
    x_tail(odd, 1).wait_recv()
    if star:
        set_factor(top[1])
    x_last(1)
    x_turn(odd * (nx - 1))

    if star:
        @pl.when(jnp.logical_not(root))
        def _():
            cast(0).wait_recv()
            set_factor(top[2])
    else:
        next_top(2)
        set_factor(top[3])
    factor = jnp.broadcast_to(top[4], (ROWS, lanes))

    @pl.loop(0, nx)
    def _(i):
        for t in range(tiles):
            r = t * ROWS
            row = pl.multiple_of(i * ny + r, ROWS)
            for field in range(5):
                state = cx[field, pl.ds(pl.multiple_of(row + 3 * ny, ROWS), ROWS), :]
                out[field, i, pl.ds(r, ROWS), :] = (1.0 / scale) * state - factor * acc[field, pl.ds(row, ROWS), :]

    if star:
        pl.when(rank == roots[0])(lambda: slots(1, top_send, top_recv).wait_send())
        pl.when(rank == roots[1])(lambda: slots(devices - 1, top_send, top_recv).wait_send())
        pl.when(jnp.logical_not(root))(lambda: slots(2, top_send, top_recv).wait_send())
    remote(hx, hx, x_send, x_recv.at[0], near(0, 1)).wait_send()
    edges = cx.at[0, pl.ds(0, 2 * (sy.shape[1] + sz.shape[1]))]
    remote(edges, edges, edge_send, z_recv, near(2, 1)).wait_send()


def local(counts, density, velocity, pressure):
    nx, ny, nz = density.shape
    nrow = nx * ny
    slots = math.prod(counts) if is_star(counts) else sum(counts) - 3
    hands = [pltpu.SemaphoreType.DMA if is_star(counts) else pltpu.SemaphoreType.DMA((slots,))] * 2
    f32 = jnp.float32
    vmem = pl.BlockSpec(memory_space=pltpu.VMEM)
    edge = pl.cdiv(15 * nx, ROWS) * ROWS
    return pl.pallas_call(
        functools.partial(kernel, counts),
        out_shape=pltpu.VMEM((5, nx, ny, nz), f32),
        in_specs=[pl.BlockSpec(memory_space=pl.ANY)] * 3,
        out_specs=vmem,
        scratch_shapes=[
            pltpu.VMEM((5, nx, ny, nz), f32),
            pltpu.VMEM((15, (nx + 6) * ny + ROWS, nz), f32),
            pltpu.VMEM((15, nx * (ny + 2 * ROWS) + ROWS, nz), f32),
            pltpu.VMEM((15, nz + 3 * ROWS, nrow), f32),
            pltpu.VMEM((5, (nx + 1) * ny, nz), f32),
            pltpu.VMEM((5, nx * (ny + 2 * ROWS), nz), f32),
            pltpu.VMEM((5, nz + ROWS, nrow), f32),
            pltpu.VMEM((5, nrow, nz), f32),
            pltpu.VMEM((5, nz, nrow), f32),
            pltpu.VMEM((2, 5, 3, ny, nz), f32),
            pltpu.VMEM((2, edge, nz), f32),
            pltpu.VMEM((2, edge, nz), f32),
            pltpu.VMEM((2, 2 * ROWS, nrow), f32),
            pltpu.VMEM((2, 2 * ROWS, nrow), f32),
            pltpu.VMEM((5, 1, nz), f32),
            pltpu.VMEM((slots, 1, nz), f32),
            pltpu.SemaphoreType.DMA,
            pltpu.SemaphoreType.DMA((8,)),
            pltpu.SemaphoreType.DMA,
            pltpu.SemaphoreType.DMA((2,)),
            pltpu.SemaphoreType.DMA,
            *hands,
            pltpu.SemaphoreType.DMA,
            pltpu.SemaphoreType.REGULAR((2,)),
        ],
        compiler_params=pltpu.CompilerParams(collective_id=0, has_side_effects=True),
    )(density, velocity, pressure)


def solution(mesh):
    counts = tuple(mesh.shape[a] for a in AXES)
    in_specs = (P("gx", "gy", "gz"), P(None, "gx", "gy", "gz"), P("gx", "gy", "gz"))
    out_specs = P(None, "gx", "gy", "gz")
    return jax.shard_map(
        functools.partial(local, counts), mesh=mesh, in_specs=in_specs, out_specs=out_specs, check_vma=False
    )
```
